32 devices in a mesh: data: 1 (over z), col: 4 (over y), row: 8 (over x, core).
Axes of the slice: x: 4, y: 4, z: 1, core: 2. Of those that a mesh axis runs over, the one named last changes fastest.
The devices are a block of a 4x4x8 slice.
Arguments:
- image: bfloat16 [256, 128, 3], P(('data', 'row'), 'col')
- w_enc1a: bfloat16 [3, 3, 3, 192], replicated
- b_enc1a: float32 [192], replicated
- w_enc1b: bfloat16 [3, 3, 192, 192], replicated
- b_enc1b: float32 [192], replicated
- w_enc2a: bfloat16 [3, 3, 192, 384], replicated
- b_enc2a: float32 [384], replicated
- w_enc2b: bfloat16 [3, 3, 384, 384], replicated
- b_enc2b: float32 [384], replicated
- w_mid_a: bfloat16 [3, 3, 384, 768], replicated
- b_mid_a: float32 [768], replicated
- w_mid_b: bfloat16 [3, 3, 768, 768], replicated
- b_mid_b: float32 [768], replicated
- w_up2: bfloat16 [2, 2, 768, 384], replicated
- w_dec2a: bfloat16 [3, 3, 768, 384], replicated
- b_dec2a: float32 [384], replicated
- w_dec2b: bfloat16 [3, 3, 384, 384], replicated
- b_dec2b: float32 [384], replicated
- w_up1: bfloat16 [2, 2, 384, 192], replicated
- w_dec1a: bfloat16 [3, 3, 384, 192], replicated
- b_dec1a: float32 [192], replicated
- w_dec1b: bfloat16 [3, 3, 192, 192], replicated
- b_dec1b: float32 [192], replicated
- w_head: bfloat16 [192, 6], replicated
- b_head: float32 [6], replicated
Outputs:
- output: float32 [256, 128, 6], P(('data', 'row'), 'col')
All inputs are finite; a program needn't handle non-finite values.
Results may differ from the reference program's by a relative error of at most 0.0159219.
Values are sent between devices in bfloat16 or wider.
A program may use at most 768 MiB of HBM per device.

```python
import jax
import jax.numpy as jnp
from jax import lax

IN_CH = 3
BASE_CH = 192
OUT_CH = 6
IMG_ROWS = 256
IMG_COLS = 128


def weight_specs():
    ch_one = BASE_CH
    ch_two = 2 * BASE_CH
    ch_four = 4 * BASE_CH
    bias_gain = 0.0625
    return [
        ("w_enc1a", (3, 3, IN_CH, ch_one), 9 * IN_CH, 2.0, jnp.bfloat16),
        ("b_enc1a", (ch_one,), 1, bias_gain, jnp.float32),
        ("w_enc1b", (3, 3, ch_one, ch_one), 9 * ch_one, 2.0, jnp.bfloat16),
        ("b_enc1b", (ch_one,), 1, bias_gain, jnp.float32),
        ("w_enc2a", (3, 3, ch_one, ch_two), 9 * ch_one, 2.0, jnp.bfloat16),
        ("b_enc2a", (ch_two,), 1, bias_gain, jnp.float32),
        ("w_enc2b", (3, 3, ch_two, ch_two), 9 * ch_two, 2.0, jnp.bfloat16),
        ("b_enc2b", (ch_two,), 1, bias_gain, jnp.float32),
        ("w_mid_a", (3, 3, ch_two, ch_four), 9 * ch_two, 2.0, jnp.bfloat16),
        ("b_mid_a", (ch_four,), 1, bias_gain, jnp.float32),
        ("w_mid_b", (3, 3, ch_four, ch_four), 9 * ch_four, 2.0, jnp.bfloat16),
        ("b_mid_b", (ch_four,), 1, bias_gain, jnp.float32),
        ("w_up2", (2, 2, ch_four, ch_two), ch_four, 1.0, jnp.bfloat16),
        ("w_dec2a", (3, 3, ch_four, ch_two), 9 * ch_four, 2.0, jnp.bfloat16),
        ("b_dec2a", (ch_two,), 1, bias_gain, jnp.float32),
        ("w_dec2b", (3, 3, ch_two, ch_two), 9 * ch_two, 2.0, jnp.bfloat16),
        ("b_dec2b", (ch_two,), 1, bias_gain, jnp.float32),
        ("w_up1", (2, 2, ch_two, ch_one), ch_two, 1.0, jnp.bfloat16),
        ("w_dec1a", (3, 3, ch_two, ch_one), 9 * ch_two, 2.0, jnp.bfloat16),
        ("b_dec1a", (ch_one,), 1, bias_gain, jnp.float32),
        ("w_dec1b", (3, 3, ch_one, ch_one), 9 * ch_one, 2.0, jnp.bfloat16),
        ("b_dec1b", (ch_one,), 1, bias_gain, jnp.float32),
        ("w_head", (ch_one, OUT_CH), ch_one, 1.0, jnp.bfloat16),
        ("b_head", (OUT_CH,), 1, bias_gain, jnp.float32),
    ]


def setup_inputs(seed: int = 0, part: int = 0) -> dict:
    root = jax.random.key(seed)
    image_key = jax.random.fold_in(jax.random.fold_in(root, 1000), part)
    pixels = jax.random.normal(image_key, (IMG_ROWS, IMG_COLS, IN_CH), jnp.float32)
    result = {"image": pixels.astype(jnp.bfloat16)}
    for index, spec in enumerate(weight_specs()):
        name, shape, fan_in, gain, dtype = spec
        values = jax.random.normal(jax.random.fold_in(root, index), shape, jnp.float32)
        result[name] = (values * (gain / fan_in) ** 0.5).astype(dtype)
    return result


def conv_relu(hidden, weight, bias):
    conv_out = lax.conv_general_dilated(hidden.astype(jnp.float32)[None], weight.astype(jnp.float32), (1, 1), "SAME", dimension_numbers=("NHWC", "HWIO", "NHWC"))[0]
    return jax.nn.relu(conv_out + bias).astype(jnp.bfloat16)


def double_conv(hidden, w_first, b_first, w_second, b_second):
    return conv_relu(conv_relu(hidden, w_first, b_first), w_second, b_second)


def max_pool(hidden):
    height, width, channels = hidden.shape
    return hidden.reshape(height // 2, 2, width // 2, 2, channels).max(axis=(1, 3))


def up_conv(hidden, weight):
    height = hidden.shape[0]
    width = hidden.shape[1]
    summed = jnp.einsum("ijc,abco->iajbo", hidden.astype(jnp.float32), weight.astype(jnp.float32))
    return summed.astype(jnp.bfloat16).reshape(2 * height, 2 * width, weight.shape[3])


def reference(image, w_enc1a, b_enc1a, w_enc1b, b_enc1b, w_enc2a, b_enc2a, w_enc2b, b_enc2b, w_mid_a, b_mid_a, w_mid_b, b_mid_b, w_up2, w_dec2a, b_dec2a, w_dec2b, b_dec2b, w_up1, w_dec1a, b_dec1a, w_dec1b, b_dec1b, w_head, b_head):
    skip_one = double_conv(image, w_enc1a, b_enc1a, w_enc1b, b_enc1b)
    skip_two = double_conv(max_pool(skip_one), w_enc2a, b_enc2a, w_enc2b, b_enc2b)
    middle = double_conv(max_pool(skip_two), w_mid_a, b_mid_a, w_mid_b, b_mid_b)
    hidden = double_conv(jnp.concatenate([up_conv(middle, w_up2), skip_two], axis=2), w_dec2a, b_dec2a, w_dec2b, b_dec2b)
    hidden = double_conv(jnp.concatenate([up_conv(hidden, w_up1), skip_one], axis=2), w_dec1a, b_dec1a, w_dec1b, b_dec1b)
    flat = hidden.reshape(-1, hidden.shape[2])
    head_out = jnp.dot(flat, w_head, preferred_element_type=jnp.float32) + b_head
    return head_out.reshape(hidden.shape[0], hidden.shape[1], w_head.shape[1])
```

```python
import functools

import jax
import jax.numpy as jnp
from jax import lax
from jax.experimental import pallas as pl
from jax.experimental.pallas import tpu as pltpu
from jax.sharding import PartitionSpec as P

MESH = pl.DeviceIdType.MESH
BF = jnp.bfloat16
F32 = jnp.float32
NORTH, SOUTH, WEST, EAST, NW, NE, SW, SE = range(8)
STEP = ((-1, 0), (1, 0), (0, -1), (0, 1), (-1, -1), (-1, 1), (1, -1), (1, 1))
OPPOSITE = (SOUTH, NORTH, EAST, WEST, SE, SW, NE, NW)
WEIGHTS = ("enc1b", "enc2a", "enc2b", "mid_a", "mid_b", "up2", "dec2a", "dec2b", "up1", "dec1a", "dec1b")
BIASES = ("enc1a", "enc1b", "enc2a", "enc2b", "mid_a", "mid_b", "dec2a", "dec2b", "dec1a", "dec1b", "head")
EXCHANGES = (("x", 8, 3), ("a1", 8, 192), ("s1", 8, 192), ("p1", 4, 192), ("a2", 4, 384), ("s2", 4, 384), ("p2", 2, 384),
             ("ma", 2, 768), ("u2", 4, 384), ("e2", 4, 384), ("u1", 8, 192), ("e1", 8, 192))


def turn(value, shift):
    shift = shift % 16
    return value if shift == 0 else pltpu.roll(value, shift, 0)


def body(rows, cols, *refs):
    refs = list(refs)

    def take(count):
        head = refs[:count]
        del refs[:count]
        return head

    x_ref, w_enc1a, w_head = take(3)
    w_hbm = dict(zip(WEIGHTS, take(len(WEIGHTS))))
    bias = dict(zip(BIASES, take(len(BIASES))))
    (y_ref,) = take(1)
    w_vm = dict(zip(WEIGHTS, take(len(WEIGHTS))))
    maps = dict(zip([e[0] for e in EXCHANGES], take(len(EXCHANGES))))
    packs = dict(zip([e[0] for e in EXCHANGES], take(len(EXCHANGES))))
    lands = dict(zip([e[0] for e in EXCHANGES], take(len(EXCHANGES))))
    corners = dict(zip([e[0] for e in EXCHANGES], take(len(EXCHANGES))))
    mb, d2 = take(2)
    w_sem, send_sem, recv_sem = take(3)

    data = lax.axis_index("data")
    row = lax.axis_index("row")
    col = lax.axis_index("col")
    has_n, has_s, has_w, has_e = row > 0, row < rows - 1, col > 0, col < cols - 1
    has = (has_n, has_s, has_w, has_e, has_n & has_w, has_n & has_e, has_s & has_w, has_s & has_e)

    def neighbour(way):
        return (data, col + STEP[way][1], row + STEP[way][0])

    w_copy = {}
    for index, name in enumerate(WEIGHTS):
        w_copy[name] = pltpu.make_async_copy(w_hbm[name], w_vm[name], w_sem.at[index])
        w_copy[name].start()

    barrier = pltpu.get_barrier_semaphore()
    count = jnp.int32(0)
    for way in range(8):
        @pl.when(has[way])
        def _(way=way):
            pl.semaphore_signal(barrier, inc=1, device_id=neighbour(way), device_id_type=MESH)
        count = count + has[way].astype(jnp.int32)
    pl.semaphore_wait(barrier, count)

    sub = lax.broadcasted_iota(jnp.int32, (16, 128), 0)

    def mask(test, channels):
        s = lax.broadcasted_iota(jnp.int32, (16, channels), 0)
        return test(s)

    def copies(name, way):
        index = [e[0] for e in EXCHANGES].index(name)
        side = EXCHANGES[index][1]
        back = OPPOSITE[way]
        if way < 4:
            source, target = packs[name].at[way], lands[name].at[back]
        else:
            i = 1 if STEP[way][0] < 0 else side
            j = 1 if STEP[way][1] < 0 else side
            source, target = maps[name].at[i, j], corners[name].at[back - 4]
        return pltpu.make_async_remote_copy(
            src_ref=source, dst_ref=target, send_sem=send_sem.at[index, way], recv_sem=recv_sem.at[index, back],
            device_id=neighbour(way), device_id_type=MESH)

    def arrival(name, way):
        index = [e[0] for e in EXCHANGES].index(name)
        target = lands[name].at[way] if way < 4 else corners[name].at[way - 4]
        return pltpu.make_async_remote_copy(
            src_ref=target, dst_ref=target, send_sem=send_sem.at[index, way], recv_sem=recv_sem.at[index, way],
            device_id=neighbour(way), device_id_type=MESH)

    def geometry(name):
        entry = EXCHANGES[[e[0] for e in EXCHANGES].index(name)]
        return entry[1], entry[2]

    def load(ref, *at):
        return ref[at].astype(F32)

    def send(name):
        side, channels = geometry(name)
        m = maps[name]
        tiles = max(side // 4, 1)
        for t in range(tiles):
            across = min(side, 4)
            packed = [None] * 4
            for k in range(across):
                e = 4 * t + k
                north = load(m, 1, 1 + e)
                south = load(m, side, 1 + e)
                west = load(m, 1 + e, 1)
                east = load(m, 1 + e, side)
                parts = (turn(north, 4 * k), turn(south, 4 * k - 12), turn(west, k), turn(east, k - 3))
                for way in range(4):
                    if k == 0:
                        packed[way] = parts[way]
                    else:
                        test = (lambda s: s // 4 == k) if way < 2 else (lambda s: s % 4 == k)
                        packed[way] = jnp.where(mask(test, channels), parts[way], packed[way])
            for way in range(4):
                packs[name][way, t] = packed[way].astype(BF)
        for way in range(8):
            @pl.when(has[way])
            def _(way=way):
                copies(name, way).start()

    def receive(name):
        for way in range(8):
            @pl.when(has[way])
            def _(way=way):
                arrival(name, way).wait_recv()
        side, channels = geometry(name)
        m, land, corner = maps[name], lands[name], corners[name]
        zero = jnp.zeros((16, channels), F32)
        top = mask(lambda s: s < 4, channels)
        bottom = mask(lambda s: s >= 12, channels)
        left = mask(lambda s: s % 4 == 0, channels)
        right = mask(lambda s: s % 4 == 3, channels)

        def came(way, tile):
            return jnp.where(has[way], load(land, way, tile), zero)

        def came_corner(way):
            return jnp.where(has[way], load(corner, way - 4), zero)

        last = side - 1
        for e in range(side):
            t, k = e // 4, e % 4
            m[0, 1 + e] = jnp.where(top, turn(came(NORTH, t), -4 * k), turn(load(m, side, 1 + e), 4)).astype(BF)
            m[side + 1, 1 + e] = jnp.where(bottom, turn(came(SOUTH, t), 12 - 4 * k), turn(load(m, 1, 1 + e), -4)).astype(BF)
            m[1 + e, 0] = jnp.where(left, turn(came(WEST, t), -k), turn(load(m, 1 + e, side), 1)).astype(BF)
            m[1 + e, side + 1] = jnp.where(right, turn(came(EAST, t), 3 - k), turn(load(m, 1 + e, 1), -1)).astype(BF)
        t, k = last // 4, last % 4
        own = turn(load(m, side, side), 5)
        value = jnp.where(top, turn(came(NORTH, t), 1 - 4 * k), own)
        value = jnp.where(left, turn(came(WEST, t), 4 - k), value)
        m[0, 0] = jnp.where(top & left, turn(came_corner(NW), 1), value).astype(BF)
        own = turn(load(m, side, 1), 3)
        value = jnp.where(top, turn(came(NORTH, 0), -1), own)
        value = jnp.where(right, turn(came(EAST, t), 7 - k), value)
        m[0, side + 1] = jnp.where(top & right, turn(came_corner(NE), 7), value).astype(BF)
        own = turn(load(m, 1, side), -3)
        value = jnp.where(bottom, turn(came(SOUTH, t), 13 - 4 * k), own)
        value = jnp.where(left, turn(came(WEST, 0), -4), value)
        m[side + 1, 0] = jnp.where(bottom & left, turn(came_corner(SW), 9), value).astype(BF)
        own = turn(load(m, 1, 1), -5)
        value = jnp.where(bottom, turn(came(SOUTH, 0), 11), own)
        value = jnp.where(right, turn(came(EAST, 0), -1), value)
        m[side + 1, side + 1] = jnp.where(bottom & right, turn(came_corner(SE), 15), value).astype(BF)

    def taps(name):
        side, channels = geometry(name)
        m = maps[name]
        return [m[dy:dy + side, dx:dx + side].reshape(side * side * 16, channels) for dy in range(3) for dx in range(3)]

    def conv_sum(sources, weight, depth):
        total = None
        for name, first in sources:
            channels = geometry(name)[1]
            for t, tap in enumerate(taps(name)):
                part = jnp.dot(tap, weight[pl.ds(t * depth + first, channels), :], preferred_element_type=F32)
                total = part if total is None else total + part
        return total

    def act(total, name):
        return jnp.maximum(total + bias[name][...], 0.0).astype(BF)

    def put(name, value):
        side, channels = geometry(name)
        maps[name][1:side + 1, 1:side + 1] = value.reshape(side, side, 16, channels)

    def pool(source, target):
        side, channels = geometry(target)
        a, b = maps[source], maps[target]
        for i in range(side):
            for j in range(side):
                p, q = 1 + 2 * i, 1 + 2 * j
                b[1 + i, 1 + j] = jnp.maximum(jnp.maximum(a[p, q], a[p, q + 1]), jnp.maximum(a[p + 1, q], a[p + 1, q + 1]))

    def up(value, weight, depth, target, side):
        channels = geometry(target)[1]
        for p in range(2):
            for q in range(2):
                w = weight[pl.ds((2 * p + q) * depth, depth), :]
                out = jnp.dot(value, w, preferred_element_type=F32).astype(BF).reshape(side, side, 16, channels)
                for i in range(side):
                    for j in range(side):
                        maps[target][1 + 2 * i + p, 1 + 2 * j + q] = out[i, j]

    maps["x"][1:9, 1:9] = x_ref[...]
    send("x")
    receive("x")
    total = None
    for t, tap in enumerate(taps("x")):
        part = jnp.dot(tap, w_enc1a[t], preferred_element_type=F32)
        total = part if total is None else total + part
    put("a1", act(total, "enc1a"))
    send("a1")
    receive("a1")
    w_copy["enc1b"].wait()
    put("s1", act(conv_sum([("a1", 0)], w_vm["enc1b"], 192), "enc1b"))
    pool("s1", "p1")
    send("p1")
    send("s1")
    receive("p1")
    w_copy["enc2a"].wait()
    put("a2", act(conv_sum([("p1", 0)], w_vm["enc2a"], 192), "enc2a"))
    send("a2")
    receive("a2")
    w_copy["enc2b"].wait()
    put("s2", act(conv_sum([("a2", 0)], w_vm["enc2b"], 384), "enc2b"))
    pool("s2", "p2")
    send("p2")
    send("s2")
    receive("p2")
    w_copy["mid_a"].wait()
    put("ma", act(conv_sum([("p2", 0)], w_vm["mid_a"], 384), "mid_a"))
    send("ma")
    receive("ma")
    w_copy["mid_b"].wait()
    mb[...] = act(conv_sum([("ma", 0)], w_vm["mid_b"], 768), "mid_b")
    w_copy["up2"].wait()
    up(mb[...], w_vm["up2"], 768, "u2", 2)
    send("u2")
    receive("s2")
    receive("u2")
    w_copy["dec2a"].wait()
    put("e2", act(conv_sum([("u2", 0), ("s2", 384)], w_vm["dec2a"], 768), "dec2a"))
    send("e2")
    receive("e2")
    w_copy["dec2b"].wait()
    d2[...] = act(conv_sum([("e2", 0)], w_vm["dec2b"], 384), "dec2b")
    w_copy["up1"].wait()
    up(d2[...], w_vm["up1"], 384, "u1", 4)
    send("u1")
    receive("s1")
    receive("u1")
    w_copy["dec1a"].wait()
    put("e1", act(conv_sum([("u1", 0), ("s1", 192)], w_vm["dec1a"], 384), "dec1a"))
    send("e1")
    receive("e1")
    w_copy["dec1b"].wait()
    d1 = act(conv_sum([("e1", 0)], w_vm["dec1b"], 192), "dec1b")
    y = jnp.dot(d1, w_head[...], preferred_element_type=F32) + bias["head"][...]
    y_ref[...] = y.reshape(y_ref.shape)

    for name, _, _ in EXCHANGES:
        for way in range(8):
            @pl.when(has[way])
            def _(way=way, name=name):
                copies(name, way).wait_send()


def solution(mesh):
    rows = mesh.shape["row"]
    cols = mesh.shape["col"]
    tile_spec = P(("data", "row"), "col", None)

    def device_body(image, *params):
        names = ("w_enc1a", "b_enc1a", "w_enc1b", "b_enc1b", "w_enc2a", "b_enc2a", "w_enc2b", "b_enc2b", "w_mid_a", "b_mid_a",
                 "w_mid_b", "b_mid_b", "w_up2", "w_dec2a", "b_dec2a", "w_dec2b", "b_dec2b", "w_up1", "w_dec1a", "b_dec1a",
                 "w_dec1b", "b_dec1b", "w_head", "b_head")
        p = dict(zip(names, params))
        high, wide, depth = image.shape
        x = image.reshape(4, high // 4, 4, wide // 4, depth).transpose(1, 3, 0, 2, 4).reshape(high // 4, wide // 4, 16, depth)
        weights = [p["w_" + n].reshape(-1, p["w_" + n].shape[-1]) for n in WEIGHTS]
        biases = [p["b_" + n].reshape(1, -1) for n in BIASES]
        vmem = pl.BlockSpec(memory_space=pltpu.VMEM)
        hbm = pl.BlockSpec(memory_space=pl.ANY)
        out_channels = p["w_head"].shape[1]
        scratch = [pltpu.VMEM(w.shape, BF) for w in weights]
        scratch += [pltpu.VMEM((s + 2, s + 2, 16, c), BF) for _, s, c in EXCHANGES]
        scratch += [pltpu.VMEM((4, max(s // 4, 1), 16, c), BF) for _, s, c in EXCHANGES]
        scratch += [pltpu.VMEM((4, max(s // 4, 1), 16, c), BF) for _, s, c in EXCHANGES]
        scratch += [pltpu.VMEM((4, 16, c), BF) for _, s, c in EXCHANGES]
        scratch += [pltpu.VMEM((64, 768), BF), pltpu.VMEM((256, 384), BF)]
        scratch += [pltpu.SemaphoreType.DMA((len(WEIGHTS),)), pltpu.SemaphoreType.DMA((len(EXCHANGES), 8)),
                    pltpu.SemaphoreType.DMA((len(EXCHANGES), 8))]
        y = pl.pallas_call(
            functools.partial(body, rows, cols),
            out_shape=jax.ShapeDtypeStruct((high // 4, wide // 4, 16, out_channels), F32),
            in_specs=[vmem] * 3 + [hbm] * len(weights) + [vmem] * len(biases),
            out_specs=vmem,
            scratch_shapes=scratch,
            compiler_params=pltpu.CompilerParams(collective_id=0, has_side_effects=True, vmem_limit_bytes=62 * 1024 * 1024),
            name="unet",
        )(x, p["w_enc1a"].reshape(9, depth, -1), p["w_head"], *weights, *biases)
        y = y.reshape(high // 4, wide // 4, 4, 4, out_channels).transpose(2, 0, 3, 1, 4)
        return y.reshape(high, wide, out_channels)

    def program(image, *params):
        mapped = jax.shard_map(device_body, mesh=mesh, in_specs=(tile_spec,) + tuple([P()] * len(params)), out_specs=tile_spec, check_vma=False)
        return mapped(image, *params)

    return program
```

```python
import functools

import jax
import jax.numpy as jnp
from jax import lax
from jax.experimental import pallas as pl
from jax.experimental.pallas import tpu as pltpu
from jax.sharding import PartitionSpec as P

MESH = pl.DeviceIdType.MESH
BF = jnp.bfloat16
F32 = jnp.float32
STEP = ((-1, 0), (1, 0), (0, -1), (0, 1), (-1, -1), (-1, 1), (1, -1), (1, 1))
OPPOSITE = (1, 0, 3, 2, 7, 6, 5, 4)
WEIGHTS = ("enc1b", "enc2a", "enc2b", "mid_a", "mid_b", "up2", "dec2a", "dec2b", "up1", "dec1a", "dec1b")
TURNED = ("up1", "dec1a")
BIASES = ("enc1a", "enc1b", "enc2a", "enc2b", "mid_a", "mid_b", "dec2a", "dec2b", "dec1a", "dec1b")
MAPS = {"x": (8, 2, 128), "s1": (8, 1, 192), "p1": (4, 2, 192), "s2": (4, 1, 384), "p2": (2, 2, 384), "u2": (4, 1, 384),
        "e2": (4, 1, 384), "u1": (8, 1, 192), "e1": (8, 1, 192), "a1": (8, 1, 192), "a2": (4, 1, 384), "ma": (2, 1, 768)}
SHARED = ("x", "s1", "p1", "s2", "p2", "u2", "e2", "u1", "e1")


def tiles_of(name):
    side, ring, _ = MAPS[name]
    return max(side * ring // 4, 1)


def turn(value, shift):
    shift = shift % 16
    return value if shift == 0 else pltpu.roll(value, shift, 0)


def rows_dot(a, b):
    return lax.dot_general(a, b, (((1,), (1,)), ((), ())), preferred_element_type=F32)


def iota(shape, axis):
    return lax.broadcasted_iota(jnp.int32, shape, axis)


def body(rows, cols, *refs):
    refs = list(refs)

    def take(count):
        head = refs[:count]
        del refs[:count]
        return head

    x_ref, w_enc1a, w_head, b_head = take(4)
    w_hbm = dict(zip(WEIGHTS, take(len(WEIGHTS))))
    bias = dict(zip(BIASES, take(len(BIASES))))
    (y_ref,) = take(1)
    w_vm = dict(zip(WEIGHTS, take(len(WEIGHTS))))
    maps = dict(zip(MAPS, take(len(MAPS))))
    packs = dict(zip(SHARED, take(len(SHARED))))
    lands = dict(zip(SHARED, take(len(SHARED))))
    x27, w27, mb, d2, d1, acc1, acc2, y_rows = take(8)
    w_sem, send_sem, recv_sem = take(3)

    data = lax.axis_index("data")
    row = lax.axis_index("row")
    col = lax.axis_index("col")
    go = row >= 0
    has_n, has_s, has_w, has_e = row > 0, row < rows - 1, col > 0, col < cols - 1
    has = (has_n, has_s, has_w, has_e, has_n & has_w, has_n & has_e, has_s & has_w, has_s & has_e)

    def neighbour(way):
        return (data, col + STEP[way][1], row + STEP[way][0])

    w_copy = {}
    for index, name in enumerate(WEIGHTS):
        w_copy[name] = pltpu.make_async_copy(w_hbm[name], w_vm[name], w_sem.at[index])
        w_copy[name].start()

    barrier = pltpu.get_barrier_semaphore()
    count = jnp.int32(0)
    for way in range(8):
        @pl.when(has[way])
        def _(way=way):
            pl.semaphore_signal(barrier, inc=1, device_id=neighbour(way), device_id_type=MESH)
        count = count + has[way].astype(jnp.int32)

    def land(name, way):
        tiles = tiles_of(name)
        return lands[name].at[pl.ds(way * tiles, tiles)] if way < 4 else lands[name].at[pl.ds(4 * tiles + way - 4, 1)]

    def pack(name, way):
        tiles = tiles_of(name)
        return packs[name].at[pl.ds(way * tiles, tiles)] if way < 4 else packs[name].at[pl.ds(4 * tiles + way - 4, 1)]

    def copies(name, way):
        index = SHARED.index(name)
        back = OPPOSITE[way]
        return pltpu.make_async_remote_copy(
            src_ref=pack(name, way), dst_ref=land(name, back), send_sem=send_sem.at[index, way],
            recv_sem=recv_sem.at[index, back], device_id=neighbour(way), device_id_type=MESH)

    def arrival(name, way):
        index = SHARED.index(name)
        return pltpu.make_async_remote_copy(
            src_ref=pack(name, way), dst_ref=land(name, way), send_sem=send_sem.at[index, way],
            recv_sem=recv_sem.at[index, way], device_id=neighbour(way), device_id_type=MESH)

    def sublane(channels):
        return iota((16, channels), 0)

    def spot(name, way, i, j):
        side, ring, _ = MAPS[name]
        di, dj = STEP[way]
        i = i - (side - ring) if di > 0 else i
        j = j - (side - ring) if dj > 0 else j
        return i * side + j if dj == 0 else i * ring + j

    def span(side, ring, d):
        return range(side) if d == 0 else range(ring) if d < 0 else range(side - ring, side)

    def send(name):
        side, ring, channels = MAPS[name]
        m, tiles = maps[name], tiles_of(name)
        s = sublane(channels)
        for way in range(8):
            di, dj = STEP[way]
            packed = {}
            for i in span(side, ring, di):
                for j in span(side, ring, dj):
                    e = spot(name, way, i, j)
                    value = m[ring + i, ring + j].astype(F32)
                    edge = 4 * (3 if di > 0 else 0) + (3 if dj > 0 else 0)
                    if way < 4:
                        t, k = e // 4, e % 4
                        value = turn(value, (4 * k if dj == 0 else k) - edge)
                        test = (s >> 2) == k if dj == 0 else (s & 3) == k
                    else:
                        t, k = 0, e
                        value = turn(value, k - edge)
                        test = s == k
                    packed[t] = value if t not in packed else jnp.where(test, value, packed[t])
            for t, value in packed.items():
                packs[name][(way * tiles if way < 4 else 4 * tiles + way - 4) + t] = value.astype(BF)
        for way in range(8):
            @pl.when(has[way])
            def _(way=way):
                copies(name, way).start()

    def receive(name):
        for way in range(8):
            @pl.when(has[way])
            def _(way=way):
                arrival(name, way).wait_recv()
        side, ring, channels = MAPS[name]
        m, tiles = maps[name], tiles_of(name)
        s = sublane(channels)
        zero = jnp.zeros((16, channels), F32)

        def came(way, tile):
            value = lands[name][(way * tiles if way < 4 else 4 * tiles + way - 4) + tile].astype(F32)
            return jnp.where(has[way], value, zero)

        for i in range(-ring, side + ring):
            for j in range(-ring, side + ring):
                di = -1 if i < 0 else 1 if i >= side else 0
                dj = -1 if j < 0 else 1 if j >= side else 0
                if di == 0 and dj == 0:
                    continue
                si, sj = i % side, j % side
                value = turn(m[ring + si, ring + sj].astype(F32), -4 * di - dj)
                hb, wb = (3 if di > 0 else 0), (3 if dj > 0 else 0)
                if di:
                    way = STEP.index((di, 0))
                    e = spot(name, OPPOSITE[way], si, sj)
                    value = jnp.where((s >> 2) == hb, turn(came(way, e // 4), 4 * hb - 4 * (e % 4) - dj), value)
                if dj:
                    way = STEP.index((0, dj))
                    e = spot(name, OPPOSITE[way], si, sj)
                    value = jnp.where((s & 3) == wb, turn(came(way, e // 4), wb - 4 * di - e % 4), value)
                if di and dj:
                    way = STEP.index((di, dj))
                    e = spot(name, OPPOSITE[way], si, sj)
                    value = jnp.where(s == 4 * hb + wb, turn(came(way, 0), 4 * hb + wb - e), value)
                m[ring + i, ring + j] = value.astype(BF)

    def clear_outside(name):
        side, ring, channels = MAPS[name]
        m = maps[name]
        s = sublane(channels)
        zero = jnp.zeros((16, channels), F32)
        inside = [None] * 4
        for way, test in enumerate(((s >> 2) == 0, (s >> 2) == 3, (s & 3) == 0, (s & 3) == 3)):
            inside[way] = jnp.logical_or(jnp.logical_not(test), has[way])
        for i in range(-ring, side + ring):
            for j in range(-ring, side + ring):
                ways = [w for w, out in enumerate((i < 0, i >= side, j < 0, j >= side)) if out]
                if ways:
                    value = m[ring + i, ring + j].astype(F32)
                    for way in ways:
                        value = jnp.where(inside[way], value, zero)
                    m[ring + i, ring + j] = value.astype(BF)

    def taps(name, out_ring):
        side, ring, channels = MAPS[name]
        m, first, size = maps[name], ring - 1 - out_ring, side + 2 * out_ring
        return [m[first + dy:first + dy + size, first + dx:first + dx + size].reshape(size * size * 16, channels)
                for dy in range(3) for dx in range(3)]

    def conv_sum(name, weight, first, depth, out_ring=0):
        total = None
        channels = MAPS[name][2]
        for t, tap in enumerate(taps(name, out_ring)):
            if weight in TURNED:
                part = rows_dot(tap, w_vm[weight][pl.ds(t * 192, 192), first:first + channels])
            else:
                part = jnp.dot(tap, w_vm[weight][pl.ds(t * depth + first, channels), :], preferred_element_type=F32)
            total = part if total is None else total + part
        return total

    def act(total, name):
        return jnp.maximum(total + bias[name][...][None, :], 0.0).astype(BF)

    def put(name, value, out_ring=0):
        side, ring, channels = MAPS[name]
        size, first = side + 2 * out_ring, ring - out_ring
        maps[name][first:first + size, first:first + size] = value.reshape(size, size, 16, channels)

    def layer(target, source, weight, depth, out_ring=0):
        w_copy[weight].wait()

        @pl.when(go)
        def _():
            put(target, act(conv_sum(source, weight, 0, depth, out_ring), weight), out_ring)

    def pool(source, target):
        side, ring, channels = MAPS[target]
        a, b, first = maps[source], maps[target], MAPS[source][1]
        for i in range(side):
            for j in range(side):
                p, q = first + 2 * i, first + 2 * j
                b[ring + i, ring + j] = jnp.maximum(jnp.maximum(a[p, q], a[p, q + 1]), jnp.maximum(a[p + 1, q], a[p + 1, q + 1]))

    def up(value, weight, target):
        side, ring, channels = MAPS[target]
        depth = value.shape[1]
        w_copy[weight].wait()

        @pl.when(go)
        def _():
            for p in range(2):
                for q in range(2):
                    if weight in TURNED:
                        out = rows_dot(value[...], w_vm[weight][pl.ds((2 * p + q) * channels, channels), :])
                    else:
                        out = jnp.dot(value[...], w_vm[weight][pl.ds((2 * p + q) * depth, depth), :], preferred_element_type=F32)
                    out = out.astype(BF).reshape(side // 2, side // 2, 16, channels)
                    for i in range(side // 2):
                        for j in range(side // 2):
                            maps[target][ring + 2 * i + p, ring + 2 * j + q] = out[i, j]

    lane, low = iota((32, 128), 1), iota((32, 128), 0)
    pixels = x_ref[...].astype(F32)
    z = None
    for hb in range(4):
        pick = (((lane >> 2) & 3) == hb) & (low == 8 * (lane & 3) + (lane >> 4))
        part = jnp.dot(pixels[:, 8 * hb:8 * hb + 8, :].reshape(24, 32).astype(BF), jnp.where(pick, 1.0, 0.0).astype(BF),
                       preferred_element_type=F32)
        z = part if z is None else z + part
    spread_row, spread_lane = iota((24, 1024), 0), iota((24, 1024), 1)
    spread = ((spread_lane >> 7) == (spread_row & 7)) & ((spread_lane & 127) == (spread_row >> 3))
    z = jnp.dot(z.T.astype(BF), jnp.where(spread, 1.0, 0.0).astype(BF), preferred_element_type=F32).astype(BF)
    for hl in range(8):
        maps["x"][2 + hl, 2:10] = z[:, 128 * hl:128 * hl + 128].reshape(8, 16, 128)
    w27[...] = jnp.zeros(w27.shape, F32)
    for t in range(9):
        w27[pl.ds(3 * t, 3), :] = w_enc1a[t].astype(F32)

    pl.semaphore_wait(barrier, count)
    send("x")
    receive("x")

    def lanes_of(value, shift):
        return value if shift == 0 else pltpu.roll(value, shift, 1)

    for j in range(10):
        three = []
        for i in range(12):
            value = None
            for dx in range(3):
                part = lanes_of(maps["x"][i, j + dx].astype(F32), 3 * dx)
                value = part if value is None else value + part
            three.append(value)
        for i in range(10):
            nine = three[i] + lanes_of(three[i + 1], 9) + lanes_of(three[i + 2], 18)
            x27[i, j] = nine.astype(BF)

    @pl.when(go)
    def _():
        put("a1", act(jnp.dot(x27[...].reshape(1600, 128), w27[...].astype(BF), preferred_element_type=F32), "enc1a"), 1)

    clear_outside("a1")
    layer("s1", "a1", "enc1b", 192)
    pool("s1", "p1")
    send("p1")
    send("s1")
    receive("p1")
    layer("a2", "p1", "enc2a", 192, 1)
    clear_outside("a2")
    layer("s2", "a2", "enc2b", 384)
    pool("s2", "p2")
    send("p2")
    send("s2")
    receive("s1")
    w_copy["dec1a"].wait()

    @pl.when(go)
    def _():
        acc1[...] = conv_sum("s1", "dec1a", 192, 384)

    receive("p2")
    layer("ma", "p2", "mid_a", 384, 1)
    clear_outside("ma")
    w_copy["mid_b"].wait()

    @pl.when(go)
    def _():
        mb[...] = act(conv_sum("ma", "mid_b", 0, 768), "mid_b")

    up(mb, "up2", "u2")
    send("u2")
    receive("s2")
    w_copy["dec2a"].wait()

    @pl.when(go)
    def _():
        acc2[...] = conv_sum("s2", "dec2a", 384, 768)

    receive("u2")

    @pl.when(go)
    def _():
        put("e2", act(conv_sum("u2", "dec2a", 0, 768) + acc2[...], "dec2a"))

    send("e2")
    receive("e2")
    w_copy["dec2b"].wait()

    @pl.when(go)
    def _():
        d2[...] = act(conv_sum("e2", "dec2b", 0, 384), "dec2b")

    up(d2, "up1", "u1")
    send("u1")
    receive("u1")

    @pl.when(go)
    def _():
        put("e1", act(conv_sum("u1", "dec1a", 0, 384) + acc1[...], "dec1a"))

    send("e1")
    receive("e1")
    w_copy["dec1b"].wait()

    @pl.when(go)
    def _():
        d1[...] = act(conv_sum("e1", "dec1b", 0, 192), "dec1b")

    @pl.when(go)
    def _():
        out_channels = y_ref.shape[0]
        for hl in range(8):
            y_rows[:, hl, :] = rows_dot(w_head[...], d1[pl.ds(128 * hl, 128), :])
        k, n = iota((128, 128), 0), iota((128, 128), 1)
        pick = ((n >> 5) == ((k >> 2) & 3)) & ((n & 31) == 8 * (k & 3) + (k >> 4))
        y = jnp.dot(y_rows[...].reshape(8 * out_channels, 128), jnp.where(pick, 1.0, 0.0), precision=lax.Precision.HIGHEST,
                    preferred_element_type=F32).reshape(out_channels, 8, 128)
        for c in range(out_channels):
            for hb in range(4):
                y_ref[c, pl.ds(8 * hb, 8), :] = y[c, :, 32 * hb:32 * hb + 32] + b_head[c]

    for name in SHARED:
        for way in range(8):
            @pl.when(has[way])
            def _(way=way, name=name):
                copies(name, way).wait_send()


def solution(mesh):
    rows = mesh.shape["row"]
    cols = mesh.shape["col"]
    tile_spec = P(("data", "row"), "col", None)

    def device_body(image, *params):
        names = ("w_enc1a", "b_enc1a", "w_enc1b", "b_enc1b", "w_enc2a", "b_enc2a", "w_enc2b", "b_enc2b", "w_mid_a", "b_mid_a",
                 "w_mid_b", "b_mid_b", "w_up2", "w_dec2a", "b_dec2a", "w_dec2b", "b_dec2b", "w_up1", "w_dec1a", "b_dec1a",
                 "w_dec1b", "b_dec1b", "w_head", "b_head")
        p = dict(zip(names, params))
        high, wide, depth = image.shape
        weights = [p["w_" + n].swapaxes(2, 3) if n in TURNED else p["w_" + n] for n in WEIGHTS]
        weights = [w.reshape(-1, w.shape[-1]) for w in weights]
        biases = [p["b_" + n] for n in BIASES]
        vmem = pl.BlockSpec(memory_space=pltpu.VMEM)
        smem = pl.BlockSpec(memory_space=pltpu.SMEM)
        hbm = pl.BlockSpec(memory_space=pl.ANY)
        out_channels = p["w_head"].shape[1]
        scratch = [pltpu.VMEM(w.shape, BF) for w in weights]
        scratch += [pltpu.VMEM((s + 2 * r, s + 2 * r, 16, c), BF) for s, r, c in MAPS.values()]
        scratch += [pltpu.VMEM((4 * tiles_of(n) + 4, 16, MAPS[n][2]), BF) for n in SHARED] * 2
        scratch += [pltpu.VMEM((10, 10, 16, 128), BF), pltpu.VMEM((128, 192), F32), pltpu.VMEM((64, 768), BF),
                    pltpu.VMEM((256, 384), BF), pltpu.VMEM((1024, 192), BF), pltpu.VMEM((1024, 192), F32),
                    pltpu.VMEM((256, 384), F32), pltpu.VMEM((out_channels, 8, 128), F32)]
        scratch += [pltpu.SemaphoreType.DMA((len(WEIGHTS),)), pltpu.SemaphoreType.DMA((len(SHARED), 8)),
                    pltpu.SemaphoreType.DMA((len(SHARED), 8))]
        y = pl.pallas_call(
            functools.partial(body, rows, cols),
            out_shape=jax.ShapeDtypeStruct((out_channels, high, wide), F32),
            in_specs=[vmem] * 3 + [smem] + [hbm] * len(weights) + [vmem] * len(biases),
            out_specs=vmem,
            scratch_shapes=scratch,
            compiler_params=pltpu.CompilerParams(collective_id=0, has_side_effects=True, vmem_limit_bytes=62 * 1024 * 1024),
            name="unet",
        )(image.transpose(2, 0, 1), p["w_enc1a"].reshape(9, depth, -1), p["w_head"].T, p["b_head"], *weights, *biases)
        return y.transpose(1, 2, 0)

    def program(image, *params):
        mapped = jax.shard_map(device_body, mesh=mesh, in_specs=(tile_spec,) + tuple([P()] * len(params)), out_specs=tile_spec, check_vma=False)
        return mapped(image, *params)

    return program
```

```python
import functools

import jax
import jax.numpy as jnp
from jax import lax
from jax.experimental import pallas as pl
from jax.experimental.pallas import tpu as pltpu
from jax.sharding import PartitionSpec as P

MESH = pl.DeviceIdType.MESH
BF = jnp.bfloat16
F32 = jnp.float32
STEP = ((-1, 0), (1, 0), (0, -1), (0, 1), (-1, -1), (-1, 1), (1, -1), (1, 1))
OPPOSITE = (1, 0, 3, 2, 7, 6, 5, 4)
WEIGHTS = ("enc1b", "enc2a", "enc2b", "mid_a", "mid_b", "up2", "dec2a", "dec2b", "up1", "dec1a", "dec1b")
TURNED = ("up1", "dec1a")
BIASES = ("enc1a", "enc1b", "enc2a", "enc2b", "mid_a", "mid_b", "dec2a", "dec2b", "dec1a", "dec1b")
MAPS = {"x": (8, 2, 128), "s1": (8, 2, 192), "p1": (4, 2, 192), "s2": (4, 2, 384), "p2": (2, 2, 384), "u2": (4, 2, 384),
        "u1": (8, 2, 192), "a1": (8, 1, 192), "a2": (4, 1, 384), "ma": (2, 1, 768), "e2": (4, 1, 384), "e1": (8, 1, 192)}
SHARED = ("x", "s1", "p1", "s2", "p2", "u2", "u1")
SMALL = ("x", "w_enc1a", "w_head") + BIASES


def tiles_of(name):
    side, ring, _ = MAPS[name]
    return max(side * ring // 4, 1)


def turn(value, shift):
    shift = shift % 16
    return value if shift == 0 else pltpu.roll(value, shift, 0)


def rows_dot(a, b):
    return lax.dot_general(a, b, (((1,), (1,)), ((), ())), preferred_element_type=F32)


def iota(shape, axis):
    return lax.broadcasted_iota(jnp.int32, shape, axis)


def body(rows, cols, *refs):
    refs = list(refs)

    def take(count):
        head = refs[:count]
        del refs[:count]
        return head

    (b_head,) = take(1)
    small_hbm = dict(zip(SMALL, take(len(SMALL))))
    w_hbm = dict(zip(WEIGHTS, take(len(WEIGHTS))))
    (y_ref,) = take(1)
    small = dict(zip(SMALL, take(len(SMALL))))
    x_ref, w_enc1a, w_head, bias = small["x"], small["w_enc1a"], small["w_head"], small
    w_vm = dict(zip(WEIGHTS, take(len(WEIGHTS))))
    maps = dict(zip(MAPS, take(len(MAPS))))
    packs = dict(zip(SHARED, take(len(SHARED))))
    lands = dict(zip(SHARED, take(len(SHARED))))
    corner_packs = dict(zip(SHARED, take(len(SHARED))))
    corner_lands = dict(zip(SHARED, take(len(SHARED))))
    x27, w27, mb, d2, d1, acc1, acc2, y_rows = take(8)
    small_sem, w_sem, send_sem, recv_sem = take(4)

    data = lax.axis_index("data")
    row = lax.axis_index("row")
    col = lax.axis_index("col")
    go = row >= 0
    has_n, has_s, has_w, has_e = row > 0, row < rows - 1, col > 0, col < cols - 1
    has = (has_n, has_s, has_w, has_e, has_n & has_w, has_n & has_e, has_s & has_w, has_s & has_e)

    def neighbour(way):
        return (data, col + STEP[way][1], row + STEP[way][0])

    barrier = pltpu.get_barrier_semaphore()
    count = jnp.int32(0)
    for way in range(8):
        @pl.when(has[way])
        def _(way=way):
            pl.semaphore_signal(barrier, inc=1, device_id=neighbour(way), device_id_type=MESH)
        count = count + has[way].astype(jnp.int32)

    small_copy = {}
    for index, name in enumerate(SMALL):
        small_copy[name] = pltpu.make_async_copy(small_hbm[name], small[name], small_sem.at[index])
        small_copy[name].start()
    w_copy = {}
    for index, name in enumerate(WEIGHTS):
        w_copy[name] = pltpu.make_async_copy(w_hbm[name], w_vm[name], w_sem.at[index])

    def land(name, way):
        return lands[name].at[way] if way < 4 else corner_lands[name].at[way - 4]

    def pack(name, way):
        return packs[name].at[way] if way < 4 else corner_packs[name].at[way - 4]

    def copies(name, way):
        index = SHARED.index(name)
        back = OPPOSITE[way]
        return pltpu.make_async_remote_copy(
            src_ref=pack(name, way), dst_ref=land(name, back), send_sem=send_sem.at[index, way],
            recv_sem=recv_sem.at[index, back], device_id=neighbour(way), device_id_type=MESH)

    def arrival(name, way):
        index = SHARED.index(name)
        return pltpu.make_async_remote_copy(
            src_ref=pack(name, way), dst_ref=land(name, way), send_sem=send_sem.at[index, way],
            recv_sem=recv_sem.at[index, way], device_id=neighbour(way), device_id_type=MESH)

    def sublane(channels):
        return iota((16, channels), 0)

    def spot(name, way, i, j):
        side, ring, _ = MAPS[name]
        di, dj = STEP[way]
        i = i - (side - ring) if di > 0 else i
        j = j - (side - ring) if dj > 0 else j
        return i * side + j if dj == 0 else i * ring + j

    def span(side, ring, d):
        return range(side) if d == 0 else range(ring) if d < 0 else range(side - ring, side)

    def send(name):
        side, ring, channels = MAPS[name]
        m, tiles = maps[name], tiles_of(name)
        s = sublane(channels)
        for way in range(8):
            di, dj = STEP[way]
            packed = {}
            for i in span(side, ring, di):
                for j in span(side, ring, dj):
                    e = spot(name, way, i, j)
                    value = m[ring + i, ring + j].astype(F32)
                    edge = 4 * (3 if di > 0 else 0) + (3 if dj > 0 else 0)
                    if way < 4:
                        t, k = e // 4, e % 4
                        value = turn(value, (4 * k if dj == 0 else k) - edge)
                        test = (s >> 2) == k if dj == 0 else (s & 3) == k
                    else:
                        t, k = 0, e
                        value = turn(value, k - edge)
                        test = s == k
                    packed[t] = value if t not in packed else jnp.where(test, value, packed[t])
            for t, value in packed.items():
                if way < 4:
                    packs[name][way, t] = value.astype(BF)
                else:
                    corner_packs[name][way - 4] = value[0:8].astype(BF)
        for way in range(8):
            @pl.when(has[way])
            def _(way=way):
                copies(name, way).start()

    def receive(name):
        for way in range(8):
            @pl.when(has[way])
            def _(way=way):
                arrival(name, way).wait_recv()
        side, ring, channels = MAPS[name]
        m, tiles = maps[name], tiles_of(name)
        s = sublane(channels)
        zero = jnp.zeros((16, channels), F32)

        def came(way, tile):
            if way < 4:
                value = lands[name][way, tile].astype(F32)
            else:
                value = jnp.concatenate([corner_lands[name][way - 4].astype(F32), zero[0:8]], axis=0)
            return jnp.where(has[way], value, zero)

        for i in range(-ring, side + ring):
            for j in range(-ring, side + ring):
                di = -1 if i < 0 else 1 if i >= side else 0
                dj = -1 if j < 0 else 1 if j >= side else 0
                if di == 0 and dj == 0:
                    continue
                si, sj = i % side, j % side
                value = turn(m[ring + si, ring + sj].astype(F32), -4 * di - dj)
                hb, wb = (3 if di > 0 else 0), (3 if dj > 0 else 0)
                if di:
                    way = STEP.index((di, 0))
                    e = spot(name, OPPOSITE[way], si, sj)
                    value = jnp.where((s >> 2) == hb, turn(came(way, e // 4), 4 * hb - 4 * (e % 4) - dj), value)
                if dj:
                    way = STEP.index((0, dj))
                    e = spot(name, OPPOSITE[way], si, sj)
                    value = jnp.where((s & 3) == wb, turn(came(way, e // 4), wb - 4 * di - e % 4), value)
                if di and dj:
                    way = STEP.index((di, dj))
                    e = spot(name, OPPOSITE[way], si, sj)
                    value = jnp.where(s == 4 * hb + wb, turn(came(way, 0), 4 * hb + wb - e), value)
                m[ring + i, ring + j] = value.astype(BF)

    def clear_outside(name):
        side, ring, channels = MAPS[name]
        m = maps[name]
        s = sublane(channels)
        zero = jnp.zeros((16, channels), F32)
        inside = [None] * 4
        for way, test in enumerate(((s >> 2) == 0, (s >> 2) == 3, (s & 3) == 0, (s & 3) == 3)):
            inside[way] = jnp.logical_or(jnp.logical_not(test), has[way])
        for i in range(-ring, side + ring):
            for j in range(-ring, side + ring):
                ways = [w for w, out in enumerate((i < 0, i >= side, j < 0, j >= side)) if out]
                if ways:
                    value = m[ring + i, ring + j].astype(F32)
                    for way in ways:
                        value = jnp.where(inside[way], value, zero)
                    m[ring + i, ring + j] = value.astype(BF)

    def taps(name, out_ring):
        side, ring, channels = MAPS[name]
        m, first, size = maps[name], ring - 1 - out_ring, side + 2 * out_ring
        return [m[first + dy:first + dy + size, first + dx:first + dx + size].reshape(size * size * 16, channels)
                for dy in range(3) for dx in range(3)]

    def conv_sum(name, weight, first, depth, out_ring=0):
        total = None
        channels = MAPS[name][2]
        for t, tap in enumerate(taps(name, out_ring)):
            if weight in TURNED:
                part = rows_dot(tap, w_vm[weight][pl.ds(t * 192, 192), first:first + channels])
            else:
                part = jnp.dot(tap, w_vm[weight][pl.ds(t * depth + first, channels), :], preferred_element_type=F32)
            total = part if total is None else total + part
        return total

    def act(total, name):
        return jnp.maximum(total + bias[name][...][None, :], 0.0).astype(BF)

    def put(name, value, out_ring=0):
        side, ring, channels = MAPS[name]
        size, first = side + 2 * out_ring, ring - out_ring
        maps[name][first:first + size, first:first + size] = value.reshape(size, size, 16, channels)

    def layer(target, source, weight, depth, out_ring=0):
        w_copy[weight].wait()

        @pl.when(go)
        def _():
            put(target, act(conv_sum(source, weight, 0, depth, out_ring), weight), out_ring)

    def pool(source, target):
        side, ring, channels = MAPS[target]
        a, b, first = maps[source], maps[target], MAPS[source][1]
        for i in range(side):
            for j in range(side):
                p, q = first + 2 * i, first + 2 * j
                b[ring + i, ring + j] = jnp.maximum(jnp.maximum(a[p, q], a[p, q + 1]), jnp.maximum(a[p + 1, q], a[p + 1, q + 1]))

    def up(value, weight, target):
        side, ring, channels = MAPS[target]
        depth = value.shape[1]
        w_copy[weight].wait()

        @pl.when(go)
        def _():
            for p in range(2):
                for q in range(2):
                    if weight in TURNED:
                        out = rows_dot(value[...], w_vm[weight][pl.ds((2 * p + q) * channels, channels), :])
                    else:
                        out = jnp.dot(value[...], w_vm[weight][pl.ds((2 * p + q) * depth, depth), :], preferred_element_type=F32)
                    out = out.astype(BF).reshape(side // 2, side // 2, 16, channels)
                    for i in range(side // 2):
                        for j in range(side // 2):
                            maps[target][ring + 2 * i + p, ring + 2 * j + q] = out[i, j]

    lane, low = iota((32, 128), 1), iota((32, 128), 0)
    for name in SMALL:
        small_copy[name].wait()
    for name in WEIGHTS:
        w_copy[name].start()
    pixels = x_ref[...].astype(F32)
    z = None
    for hb in range(4):
        pick = (((lane >> 2) & 3) == hb) & (low == 8 * (lane & 3) + (lane >> 4))
        part = jnp.dot(pixels[:, 8 * hb:8 * hb + 8, :].reshape(24, 32).astype(BF), jnp.where(pick, 1.0, 0.0).astype(BF),
                       preferred_element_type=F32)
        z = part if z is None else z + part
    spread_row, spread_lane = iota((24, 1024), 0), iota((24, 1024), 1)
    spread = ((spread_lane >> 7) == (spread_row & 7)) & ((spread_lane & 127) == (spread_row >> 3))
    z = jnp.dot(z.T.astype(BF), jnp.where(spread, 1.0, 0.0).astype(BF), preferred_element_type=F32).astype(BF)
    for hl in range(8):
        maps["x"][2 + hl, 2:10] = z[:, 128 * hl:128 * hl + 128].reshape(8, 16, 128)
    w27[...] = jnp.zeros(w27.shape, F32)
    for t in range(9):
        w27[pl.ds(3 * t, 3), :] = w_enc1a[t].astype(F32)

    pl.semaphore_wait(barrier, count)
    send("x")
    receive("x")

    def lanes_of(value, shift):
        return value if shift == 0 else pltpu.roll(value, shift, 1)

    for j in range(10):
        three = []
        for i in range(12):
            value = None
            for dx in range(3):
                part = lanes_of(maps["x"][i, j + dx].astype(F32), 3 * dx)
                value = part if value is None else value + part
            three.append(value)
        for i in range(10):
            nine = three[i] + lanes_of(three[i + 1], 9) + lanes_of(three[i + 2], 18)
            x27[i, j] = nine.astype(BF)

    @pl.when(go)
    def _():
        put("a1", act(jnp.dot(x27[...].reshape(1600, 128), w27[...].astype(BF), preferred_element_type=F32), "enc1a"), 1)

    clear_outside("a1")
    layer("s1", "a1", "enc1b", 192)
    pool("s1", "p1")
    send("p1")
    receive("p1")
    send("s1")
    layer("a2", "p1", "enc2a", 192, 1)
    clear_outside("a2")
    layer("s2", "a2", "enc2b", 384)
    pool("s2", "p2")
    send("p2")
    receive("s1")
    w_copy["dec1a"].wait()

    @pl.when(go)
    def _():
        acc1[...] = conv_sum("s1", "dec1a", 192, 384, 1)

    receive("p2")
    send("s2")
    layer("ma", "p2", "mid_a", 384, 1)
    clear_outside("ma")
    w_copy["mid_b"].wait()

    @pl.when(go)
    def _():
        mb[...] = act(conv_sum("ma", "mid_b", 0, 768), "mid_b")

    up(mb, "up2", "u2")
    send("u2")
    receive("s2")
    w_copy["dec2a"].wait()

    @pl.when(go)
    def _():
        acc2[...] = conv_sum("s2", "dec2a", 384, 768, 1)

    receive("u2")

    @pl.when(go)
    def _():
        put("e2", act(conv_sum("u2", "dec2a", 0, 768, 1) + acc2[...], "dec2a"), 1)

    clear_outside("e2")
    w_copy["dec2b"].wait()

    @pl.when(go)
    def _():
        d2[...] = act(conv_sum("e2", "dec2b", 0, 384), "dec2b")

    up(d2, "up1", "u1")
    send("u1")
    receive("u1")

    @pl.when(go)
    def _():
        put("e1", act(conv_sum("u1", "dec1a", 0, 384, 1) + acc1[...], "dec1a"), 1)

    clear_outside("e1")
    w_copy["dec1b"].wait()

    @pl.when(go)
    def _():
        d1[...] = act(conv_sum("e1", "dec1b", 0, 192), "dec1b")

    @pl.when(go)
    def _():
        out_channels = y_ref.shape[0]
        for hl in range(8):
            y_rows[:, hl, :] = rows_dot(w_head[...], d1[pl.ds(128 * hl, 128), :])
        k, n = iota((128, 128), 0), iota((128, 128), 1)
        pick = ((n >> 5) == ((k >> 2) & 3)) & ((n & 31) == 8 * (k & 3) + (k >> 4))
        y = jnp.dot(y_rows[...].reshape(8 * out_channels, 128), jnp.where(pick, 1.0, 0.0), precision=lax.Precision.HIGHEST,
                    preferred_element_type=F32).reshape(out_channels, 8, 128)
        for c in range(out_channels):
            for hb in range(4):
                y_ref[c, pl.ds(8 * hb, 8), :] = y[c, :, 32 * hb:32 * hb + 32] + b_head[c]

    for name in SHARED:
        for way in range(8):
            @pl.when(has[way])
            def _(way=way, name=name):
                copies(name, way).wait_send()


def solution(mesh):
    rows = mesh.shape["row"]
    cols = mesh.shape["col"]
    tile_spec = P(("data", "row"), "col", None)

    def device_body(image, *params):
        names = ("w_enc1a", "b_enc1a", "w_enc1b", "b_enc1b", "w_enc2a", "b_enc2a", "w_enc2b", "b_enc2b", "w_mid_a", "b_mid_a",
                 "w_mid_b", "b_mid_b", "w_up2", "w_dec2a", "b_dec2a", "w_dec2b", "b_dec2b", "w_up1", "w_dec1a", "b_dec1a",
                 "w_dec1b", "b_dec1b", "w_head", "b_head")
        p = dict(zip(names, params))
        high, wide, depth = image.shape
        weights = [p["w_" + n].swapaxes(2, 3) if n in TURNED else p["w_" + n] for n in WEIGHTS]
        weights = [w.reshape(-1, w.shape[-1]) for w in weights]
        biases = [p["b_" + n] for n in BIASES]
        vmem = pl.BlockSpec(memory_space=pltpu.VMEM)
        smem = pl.BlockSpec(memory_space=pltpu.SMEM)
        hbm = pl.BlockSpec(memory_space=pl.ANY)
        out_channels = p["w_head"].shape[1]
        smalls = [image.transpose(2, 0, 1), p["w_enc1a"].reshape(9, depth, -1), p["w_head"].T] + biases
        scratch = [pltpu.VMEM(a.shape, a.dtype) for a in smalls + weights]
        scratch += [pltpu.VMEM((s + 2 * r, s + 2 * r, 16, c), BF) for s, r, c in MAPS.values()]
        scratch += [pltpu.VMEM((4, tiles_of(n), 16, MAPS[n][2]), BF) for n in SHARED] * 2
        scratch += [pltpu.VMEM((4, 8, MAPS[n][2]), BF) for n in SHARED] * 2
        scratch += [pltpu.VMEM((10, 10, 16, 128), BF), pltpu.VMEM((128, 192), F32), pltpu.VMEM((64, 768), BF),
                    pltpu.VMEM((256, 384), BF), pltpu.VMEM((1024, 192), BF), pltpu.VMEM((1600, 192), F32),
                    pltpu.VMEM((576, 384), F32), pltpu.VMEM((out_channels, 8, 128), F32)]
        scratch += [pltpu.SemaphoreType.DMA((len(SMALL),)), pltpu.SemaphoreType.DMA((len(WEIGHTS),)), pltpu.SemaphoreType.DMA((len(SHARED), 8)),
                    pltpu.SemaphoreType.DMA((len(SHARED), 8))]
        y = pl.pallas_call(
            functools.partial(body, rows, cols),
            out_shape=jax.ShapeDtypeStruct((out_channels, high, wide), F32),
            in_specs=[smem] + [hbm] * (len(smalls) + len(weights)),
            out_specs=vmem,
            scratch_shapes=scratch,
            compiler_params=pltpu.CompilerParams(collective_id=0, has_side_effects=True, vmem_limit_bytes=62 * 1024 * 1024),
            name="unet",
        )(p["b_head"], *smalls, *weights)
        return y.transpose(1, 2, 0)

    def program(image, *params):
        mapped = jax.shard_map(device_body, mesh=mesh, in_specs=(tile_spec,) + tuple([P()] * len(params)), out_specs=tile_spec, check_vma=False)
        return mapped(image, *params)

    return program
```

```python
import functools

import jax
import jax.numpy as jnp
from jax import lax
from jax.experimental import pallas as pl
from jax.experimental.pallas import tpu as pltpu
from jax.sharding import PartitionSpec as P

MESH = pl.DeviceIdType.MESH
BF = jnp.bfloat16
F32 = jnp.float32
STEP = ((-1, 0), (1, 0), (0, -1), (0, 1), (-1, -1), (-1, 1), (1, -1), (1, 1))
OPPOSITE = (1, 0, 3, 2, 7, 6, 5, 4)
WEIGHTS = ("enc1b", "enc2a", "enc2b", "mid_a", "mid_b", "up2", "dec2a", "dec2b", "up1", "dec1a", "dec1b")
TURNED = ("up1", "dec1a")
BIASES = ("enc1a", "enc1b", "enc2a", "enc2b", "mid_a", "mid_b", "dec2a", "dec2b", "dec1a", "dec1b")
MAPS = {"x": (8, 2, 128), "s1": (8, 2, 192), "p1": (4, 2, 192), "s2": (4, 2, 384), "p2": (2, 2, 384), "u2": (4, 2, 384),
        "u1": (8, 2, 192), "a1": (8, 1, 192), "a2": (4, 1, 384), "ma": (2, 1, 768), "e2": (4, 1, 384), "e1": (8, 1, 192)}
SHARED = ("x", "s1", "p1", "s2", "p2", "u2", "u1")
SMALL = ("x", "w_enc1a", "w_head") + BIASES


def tiles_of(name):
    side, ring, _ = MAPS[name]
    return max(side * ring // 4, 1)


def turn(value, shift):
    shift = shift % 16
    return value if shift == 0 else pltpu.roll(value, shift, 0)


def rows_dot(a, b):
    return lax.dot_general(a, b, (((1,), (1,)), ((), ())), preferred_element_type=F32)


def iota(shape, axis):
    return lax.broadcasted_iota(jnp.int32, shape, axis)


def body(rows, cols, *refs):
    refs = list(refs)

    def take(count):
        head = refs[:count]
        del refs[:count]
        return head

    (b_head,) = take(1)
    small_hbm = dict(zip(SMALL, take(len(SMALL))))
    w_hbm = dict(zip(WEIGHTS, take(len(WEIGHTS))))
    (y_ref,) = take(1)
    small = dict(zip(SMALL, take(len(SMALL))))
    x_ref, w_enc1a, w_head, bias = small["x"], small["w_enc1a"], small["w_head"], small
    w_vm = dict(zip(WEIGHTS, take(len(WEIGHTS))))
    maps = dict(zip(MAPS, take(len(MAPS))))
    packs = dict(zip(SHARED, take(len(SHARED))))
    lands = dict(zip(SHARED, take(len(SHARED))))
    corner_packs = dict(zip(SHARED, take(len(SHARED))))
    corner_lands = dict(zip(SHARED, take(len(SHARED))))
    x27, w27, mb, d2, d1, acc1, acc2, y_rows = take(8)
    small_sem, w_sem, send_sem, recv_sem = take(4)

    data = lax.axis_index("data")
    row = lax.axis_index("row")
    col = lax.axis_index("col")
    go = row >= 0
    has_n, has_s, has_w, has_e = row > 0, row < rows - 1, col > 0, col < cols - 1
    has = (has_n, has_s, has_w, has_e, has_n & has_w, has_n & has_e, has_s & has_w, has_s & has_e)

    def neighbour(way):
        return (data, col + STEP[way][1], row + STEP[way][0])

    barrier = pltpu.get_barrier_semaphore()
    count = jnp.int32(0)
    for way in range(8):
        @pl.when(has[way])
        def _(way=way):
            pl.semaphore_signal(barrier, inc=1, device_id=neighbour(way), device_id_type=MESH)
        count = count + has[way].astype(jnp.int32)

    small_copy = {}
    for index, name in enumerate(SMALL):
        small_copy[name] = pltpu.make_async_copy(small_hbm[name], small[name], small_sem.at[index])
        small_copy[name].start()
    w_copy = {}
    for index, name in enumerate(WEIGHTS):
        w_copy[name] = pltpu.make_async_copy(w_hbm[name], w_vm[name], w_sem.at[index])

    def land(name, way):
        return lands[name].at[way] if way < 4 else corner_lands[name].at[way - 4]

    def pack(name, way):
        return packs[name].at[way] if way < 4 else corner_packs[name].at[way - 4]

    def copies(name, way):
        index = SHARED.index(name)
        back = OPPOSITE[way]
        return pltpu.make_async_remote_copy(
            src_ref=pack(name, way), dst_ref=land(name, back), send_sem=send_sem.at[index, way],
            recv_sem=recv_sem.at[index, back], device_id=neighbour(way), device_id_type=MESH)

    def arrival(name, way):
        index = SHARED.index(name)
        return pltpu.make_async_remote_copy(
            src_ref=pack(name, way), dst_ref=land(name, way), send_sem=send_sem.at[index, way],
            recv_sem=recv_sem.at[index, way], device_id=neighbour(way), device_id_type=MESH)

    def sublane(channels):
        return iota((16, channels), 0)

    def spot(name, way, i, j):
        side, ring, _ = MAPS[name]
        di, dj = STEP[way]
        i = i - (side - ring) if di > 0 else i
        j = j - (side - ring) if dj > 0 else j
        return i * side + j if dj == 0 else i * ring + j

    def span(side, ring, d):
        return range(side) if d == 0 else range(ring) if d < 0 else range(side - ring, side)

    def send(name):
        side, ring, channels = MAPS[name]
        m, tiles = maps[name], tiles_of(name)
        s = sublane(channels)
        for way in range(8):
            di, dj = STEP[way]
            packed = {}
            for i in span(side, ring, di):
                for j in span(side, ring, dj):
                    e = spot(name, way, i, j)
                    value = m[ring + i, ring + j].astype(F32)
                    edge = 4 * (3 if di > 0 else 0) + (3 if dj > 0 else 0)
                    if way < 4:
                        t, k = e // 4, e % 4
                        value = turn(value, (4 * k if dj == 0 else k) - edge)
                        test = (s >> 2) == k if dj == 0 else (s & 3) == k
                    else:
                        t, k = 0, e
                        value = turn(value, k - edge)
                        test = s == k
                    packed[t] = value if t not in packed else jnp.where(test, value, packed[t])
            for t, value in packed.items():
                if way < 4:
                    packs[name][way, t] = value.astype(BF)
                else:
                    corner_packs[name][way - 4] = value[0:8].astype(BF)
        for way in range(8):
            @pl.when(has[way])
            def _(way=way):
                copies(name, way).start()

    def receive(name):
        for way in range(8):
            @pl.when(has[way])
            def _(way=way):
                arrival(name, way).wait_recv()
        side, ring, channels = MAPS[name]
        m, tiles = maps[name], tiles_of(name)
        s = sublane(channels)
        zero = jnp.zeros((16, channels), F32)

        def came(way, tile):
            if way < 4:
                value = lands[name][way, tile].astype(F32)
            else:
                value = jnp.concatenate([corner_lands[name][way - 4].astype(F32), zero[0:8]], axis=0)
            return jnp.where(has[way], value, zero)

        for i in range(-ring, side + ring):
            for j in range(-ring, side + ring):
                di = -1 if i < 0 else 1 if i >= side else 0
                dj = -1 if j < 0 else 1 if j >= side else 0
                if di == 0 and dj == 0:
                    continue
                si, sj = i % side, j % side
                value = turn(m[ring + si, ring + sj].astype(F32), -4 * di - dj)
                hb, wb = (3 if di > 0 else 0), (3 if dj > 0 else 0)
                if di:
                    way = STEP.index((di, 0))
                    e = spot(name, OPPOSITE[way], si, sj)
                    value = jnp.where((s >> 2) == hb, turn(came(way, e // 4), 4 * hb - 4 * (e % 4) - dj), value)
                if dj:
                    way = STEP.index((0, dj))
                    e = spot(name, OPPOSITE[way], si, sj)
                    value = jnp.where((s & 3) == wb, turn(came(way, e // 4), wb - 4 * di - e % 4), value)
                if di and dj:
                    way = STEP.index((di, dj))
                    e = spot(name, OPPOSITE[way], si, sj)
                    value = jnp.where(s == 4 * hb + wb, turn(came(way, 0), 4 * hb + wb - e), value)
                m[ring + i, ring + j] = value.astype(BF)

    def clear_outside(name):
        side, ring, channels = MAPS[name]
        m = maps[name]
        s = sublane(channels)
        zero = jnp.zeros((16, channels), F32)
        inside = [None] * 4
        for way, test in enumerate(((s >> 2) == 0, (s >> 2) == 3, (s & 3) == 0, (s & 3) == 3)):
            inside[way] = jnp.logical_or(jnp.logical_not(test), has[way])
        for i in range(-ring, side + ring):
            for j in range(-ring, side + ring):
                ways = [w for w, out in enumerate((i < 0, i >= side, j < 0, j >= side)) if out]
                if ways:
                    value = m[ring + i, ring + j].astype(F32)
                    for way in ways:
                        value = jnp.where(inside[way], value, zero)
                    m[ring + i, ring + j] = value.astype(BF)

    def taps(name, out_ring):
        side, ring, channels = MAPS[name]
        m, first, size = maps[name], ring - 1 - out_ring, side + 2 * out_ring
        return [m[first + dy:first + dy + size, first + dx:first + dx + size].reshape(size * size * 16, channels)
                for dy in range(3) for dx in range(3)]

    def tap_weight(weight, t, count, first, channels, depth):
        if depth == channels:
            return w_vm[weight][pl.ds(t * depth, count * depth), :]
        parts = [w_vm[weight][pl.ds(u * depth + first, channels), :] for u in range(t, t + count)]
        return parts[0] if count == 1 else jnp.concatenate(parts, axis=0)

    def chain(values, numbers, weight, first, channels, depth):
        total, at = None, 0
        while at < len(values):
            count = 1
            if channels == 384 and weight not in TURNED:
                while count < 2 and at + count < len(values) and numbers[at + count] == numbers[at] + count:
                    count += 1
            value = values[at] if count == 1 else jnp.concatenate(values[at:at + count], axis=1)
            if weight in TURNED:
                part = rows_dot(value, w_vm[weight][pl.ds(numbers[at] * 192, 192), first:first + channels])
            else:
                part = jnp.dot(value, tap_weight(weight, numbers[at], count, first, channels, depth), preferred_element_type=F32)
            total = part if total is None else total + part
            at += count
        return total

    def conv_sum(name, weight, first, depth, out_ring=0):
        return chain(taps(name, out_ring), range(9), weight, first, MAPS[name][2], depth)

    def clear_ring(name):
        side, ring, channels = MAPS[name]
        m, wide = maps[name], side + 2 * ring
        flat, tall = jnp.zeros((ring, wide, 16, channels), BF), jnp.zeros((side, ring, 16, channels), BF)
        m[0:ring] = flat
        m[side + ring:wide] = flat
        m[ring:side + ring, 0:ring] = tall
        m[ring:side + ring, side + ring:wide] = tall

    def ring_sum(name, weight, first, depth, acc):
        side, ring, channels = MAPS[name]
        m, size = maps[name], side + 2
        lines = ((0, 1), (0, size - 1), (size - 2, size - 1))
        blank = jnp.zeros((2, 16, channels), BF)

        def product(values, numbers):
            values = [v.reshape(2 * size * 16, channels) for v in values]
            return chain(values, numbers, weight, first, channels, depth).reshape(2, size, 16, -1)

        for dy in range(3):
            out = product([jnp.concatenate([m[r + dy, dx:dx + size] for r in lines[dy]], axis=0) for dx in range(3)],
                          [3 * dy + dx for dx in range(3)])
            for n, r in enumerate(lines[dy]):
                acc[r] = acc[r] + out[n]
        for dx in range(3):
            strips = [jnp.concatenate([blank, m[2:side + 2, r + dx], blank], axis=0) for r in lines[dx]]
            out = product([jnp.concatenate([strip[dy:dy + size] for strip in strips], axis=0) for dy in range(3)],
                          [3 * dy + dx for dy in range(3)])
            for n, r in enumerate(lines[dx]):
                acc[:, r] = acc[:, r] + out[n]

    def act(total, name):
        return jnp.maximum(total + bias[name][...][None, :], 0.0).astype(BF)

    def put(name, value, out_ring=0):
        side, ring, channels = MAPS[name]
        size, first = side + 2 * out_ring, ring - out_ring
        maps[name][first:first + size, first:first + size] = value.reshape(size, size, 16, channels)

    def layer(target, source, weight, depth, out_ring=0):
        w_copy[weight].wait()

        @pl.when(go)
        def _():
            put(target, act(conv_sum(source, weight, 0, depth, out_ring), weight), out_ring)

    def pool(source, target):
        side, ring, channels = MAPS[target]
        a, b, first = maps[source], maps[target], MAPS[source][1]
        for i in range(side):
            for j in range(side):
                p, q = first + 2 * i, first + 2 * j
                b[ring + i, ring + j] = jnp.maximum(jnp.maximum(a[p, q], a[p, q + 1]), jnp.maximum(a[p + 1, q], a[p + 1, q + 1]))

    def up(value, weight, target):
        side, ring, channels = MAPS[target]
        depth = value.shape[1]
        w_copy[weight].wait()

        @pl.when(go)
        def _():
            for p in range(2):
                for q in range(2):
                    if weight in TURNED:
                        out = rows_dot(value[...], w_vm[weight][pl.ds((2 * p + q) * channels, channels), :])
                    else:
                        out = jnp.dot(value[...], w_vm[weight][pl.ds((2 * p + q) * depth, depth), :], preferred_element_type=F32)
                    out = out.astype(BF).reshape(side // 2, side // 2, 16, channels)
                    for i in range(side // 2):
                        for j in range(side // 2):
                            maps[target][ring + 2 * i + p, ring + 2 * j + q] = out[i, j]

    lane, low = iota((32, 128), 1), iota((32, 128), 0)
    for name in SMALL:
        small_copy[name].wait()
    for name in WEIGHTS:
        w_copy[name].start()
    pixels = x_ref[...].astype(F32)
    z = None
    for hb in range(4):
        pick = (((lane >> 2) & 3) == hb) & (low == 8 * (lane & 3) + (lane >> 4))
        part = jnp.dot(pixels[:, 8 * hb:8 * hb + 8, :].reshape(24, 32).astype(BF), jnp.where(pick, 1.0, 0.0).astype(BF),
                       preferred_element_type=F32)
        z = part if z is None else z + part
    spread_row, spread_lane = iota((24, 1024), 0), iota((24, 1024), 1)
    spread = ((spread_lane >> 7) == (spread_row & 7)) & ((spread_lane & 127) == (spread_row >> 3))
    z = jnp.dot(z.T.astype(BF), jnp.where(spread, 1.0, 0.0).astype(BF), preferred_element_type=F32).astype(BF)
    for hl in range(8):
        maps["x"][2 + hl, 2:10] = z[:, 128 * hl:128 * hl + 128].reshape(8, 16, 128)
    w27[...] = jnp.zeros(w27.shape, F32)
    for t in range(9):
        w27[pl.ds(3 * t, 3), :] = w_enc1a[t].astype(F32)

    pl.semaphore_wait(barrier, count)
    send("x")
    clear_ring("u1")
    clear_ring("p1")
    receive("x")

    def lanes_of(value, shift):
        return value if shift == 0 else pltpu.roll(value, shift, 1)

    for j in range(10):
        three = []
        for i in range(12):
            value = None
            for dx in range(3):
                part = lanes_of(maps["x"][i, j + dx].astype(F32), 3 * dx)
                value = part if value is None else value + part
            three.append(value)
        for i in range(10):
            nine = three[i] + lanes_of(three[i + 1], 9) + lanes_of(three[i + 2], 18)
            x27[i, j] = nine.astype(BF)

    @pl.when(go)
    def _():
        put("a1", act(jnp.dot(x27[...].reshape(1600, 128), w27[...].astype(BF), preferred_element_type=F32), "enc1a"), 1)

    clear_outside("a1")
    layer("s1", "a1", "enc1b", 192)
    pool("s1", "p1")
    send("p1")
    w_copy["enc2a"].wait()

    @pl.when(go)
    def _():
        acc2[...] = conv_sum("p1", "enc2a", 0, 192, 1).reshape(acc2.shape)

    receive("p1")
    send("s1")

    @pl.when(go)
    def _():
        ring_sum("p1", "enc2a", 0, 192, acc2)

    @pl.when(go)
    def _():
        put("a2", act(acc2[...].reshape(576, 384), "enc2a"), 1)

    clear_outside("a2")
    layer("s2", "a2", "enc2b", 384)
    pool("s2", "p2")
    send("p2")
    receive("s1")
    w_copy["dec1a"].wait()

    @pl.when(go)
    def _():
        acc1[...] = conv_sum("s1", "dec1a", 192, 384, 1).reshape(acc1.shape)

    receive("p2")
    send("s2")
    layer("ma", "p2", "mid_a", 384, 1)
    clear_outside("ma")
    w_copy["mid_b"].wait()

    @pl.when(go)
    def _():
        mb[...] = act(conv_sum("ma", "mid_b", 0, 768), "mid_b")

    up(mb, "up2", "u2")
    send("u2")
    receive("s2")
    w_copy["dec2a"].wait()

    @pl.when(go)
    def _():
        acc2[...] = conv_sum("s2", "dec2a", 384, 768, 1).reshape(acc2.shape)

    receive("u2")

    @pl.when(go)
    def _():
        put("e2", act(conv_sum("u2", "dec2a", 0, 768, 1) + acc2[...].reshape(576, 384), "dec2a"), 1)

    clear_outside("e2")
    w_copy["dec2b"].wait()

    @pl.when(go)
    def _():
        d2[...] = act(conv_sum("e2", "dec2b", 0, 384), "dec2b")

    up(d2, "up1", "u1")
    send("u1")

    @pl.when(go)
    def _():
        acc1[...] = acc1[...] + conv_sum("u1", "dec1a", 0, 384, 1).reshape(acc1.shape)

    receive("u1")

    @pl.when(go)
    def _():
        ring_sum("u1", "dec1a", 0, 384, acc1)

    @pl.when(go)
    def _():
        put("e1", act(acc1[...].reshape(1600, 192), "dec1a"), 1)

    clear_outside("e1")
    w_copy["dec1b"].wait()

    @pl.when(go)
    def _():
        d1[...] = act(conv_sum("e1", "dec1b", 0, 192), "dec1b")

    @pl.when(go)
    def _():
        out_channels = y_ref.shape[0]
        for hl in range(8):
            y_rows[:, hl, :] = rows_dot(w_head[...], d1[pl.ds(128 * hl, 128), :])
        k, n = iota((128, 128), 0), iota((128, 128), 1)
        pick = ((n >> 5) == ((k >> 2) & 3)) & ((n & 31) == 8 * (k & 3) + (k >> 4))
        y = jnp.dot(y_rows[...].reshape(8 * out_channels, 128), jnp.where(pick, 1.0, 0.0), precision=lax.Precision.HIGHEST,
                    preferred_element_type=F32).reshape(out_channels, 8, 128)
        for c in range(out_channels):
            for hb in range(4):
                y_ref[c, pl.ds(8 * hb, 8), :] = y[c, :, 32 * hb:32 * hb + 32] + b_head[c]

    for name in SHARED:
        for way in range(8):
            @pl.when(has[way])
            def _(way=way, name=name):
                copies(name, way).wait_send()


def solution(mesh):
    rows = mesh.shape["row"]
    cols = mesh.shape["col"]
    tile_spec = P(("data", "row"), "col", None)

    def device_body(image, *params):
        names = ("w_enc1a", "b_enc1a", "w_enc1b", "b_enc1b", "w_enc2a", "b_enc2a", "w_enc2b", "b_enc2b", "w_mid_a", "b_mid_a",
                 "w_mid_b", "b_mid_b", "w_up2", "w_dec2a", "b_dec2a", "w_dec2b", "b_dec2b", "w_up1", "w_dec1a", "b_dec1a",
                 "w_dec1b", "b_dec1b", "w_head", "b_head")
        p = dict(zip(names, params))
        high, wide, depth = image.shape
        weights = [p["w_" + n].swapaxes(2, 3) if n in TURNED else p["w_" + n] for n in WEIGHTS]
        weights = [w.reshape(-1, w.shape[-1]) for w in weights]
        biases = [p["b_" + n] for n in BIASES]
        vmem = pl.BlockSpec(memory_space=pltpu.VMEM)
        smem = pl.BlockSpec(memory_space=pltpu.SMEM)
        hbm = pl.BlockSpec(memory_space=pl.ANY)
        out_channels = p["w_head"].shape[1]
        smalls = [image.transpose(2, 0, 1), p["w_enc1a"].reshape(9, depth, -1), p["w_head"].T] + biases
        scratch = [pltpu.VMEM(a.shape, a.dtype) for a in smalls + weights]
        scratch += [pltpu.VMEM((s + 2 * r, s + 2 * r, 16, c), BF) for s, r, c in MAPS.values()]
        scratch += [pltpu.VMEM((4, tiles_of(n), 16, MAPS[n][2]), BF) for n in SHARED] * 2
        scratch += [pltpu.VMEM((4, 8, MAPS[n][2]), BF) for n in SHARED] * 2
        scratch += [pltpu.VMEM((10, 10, 16, 128), BF), pltpu.VMEM((128, 192), F32), pltpu.VMEM((64, 768), BF),
                    pltpu.VMEM((256, 384), BF), pltpu.VMEM((1024, 192), BF), pltpu.VMEM((10, 10, 16, 192), F32),
                    pltpu.VMEM((6, 6, 16, 384), F32), pltpu.VMEM((out_channels, 8, 128), F32)]
        scratch += [pltpu.SemaphoreType.DMA((len(SMALL),)), pltpu.SemaphoreType.DMA((len(WEIGHTS),)), pltpu.SemaphoreType.DMA((len(SHARED), 8)),
                    pltpu.SemaphoreType.DMA((len(SHARED), 8))]
        y = pl.pallas_call(
            functools.partial(body, rows, cols),
            out_shape=jax.ShapeDtypeStruct((out_channels, high, wide), F32),
            in_specs=[smem] + [hbm] * (len(smalls) + len(weights)),
            out_specs=vmem,
            scratch_shapes=scratch,
            compiler_params=pltpu.CompilerParams(collective_id=0, has_side_effects=True, vmem_limit_bytes=62 * 1024 * 1024),
            name="unet",
        )(p["b_head"], *smalls, *weights)
        return y.transpose(1, 2, 0)

    def program(image, *params):
        mapped = jax.shard_map(device_body, mesh=mesh, in_specs=(tile_spec,) + tuple([P()] * len(params)), out_specs=tile_spec, check_vma=False)
        return mapped(image, *params)

    return program
```

```python
import functools

import jax
import jax.numpy as jnp
from jax import lax
from jax.experimental import pallas as pl
from jax.experimental.pallas import tpu as pltpu
from jax.sharding import PartitionSpec as P

MESH = pl.DeviceIdType.MESH
BF = jnp.bfloat16
F32 = jnp.float32
STEP = ((-1, 0), (1, 0), (0, -1), (0, 1), (-1, -1), (-1, 1), (1, -1), (1, 1))
OPPOSITE = (1, 0, 3, 2, 7, 6, 5, 4)
ORDER = (2, 3, 4, 5, 6, 7, 0, 1)
WEIGHTS = ("enc1b", "enc2a", "enc2b", "mid_a", "mid_b", "up2", "dec2a", "dec2b", "up1", "dec1a", "dec1b")
TURNED = ("up1", "dec1a")
BIASES = ("enc1a", "enc1b", "enc2a", "enc2b", "mid_a", "mid_b", "dec2a", "dec2b", "dec1a", "dec1b")
MAPS = {"x": (8, 2, 128), "s1": (8, 2, 192), "p1": (4, 2, 192), "s2": (4, 2, 384), "p2": (2, 2, 384), "u2": (4, 2, 384),
        "u1": (8, 2, 192), "a1": (8, 1, 192), "a2": (4, 1, 384), "ma": (2, 1, 768), "e2": (4, 1, 384), "e1": (8, 1, 192)}
SHARED = ("x", "s1", "p1", "s2", "p2", "u2", "u1")
SMALL = ("x", "w_enc1a", "w_head") + BIASES


def tiles_of(name):
    side, ring, _ = MAPS[name]
    return max(side * ring // 4, 1)


def turn(value, shift):
    shift = shift % 16
    return value if shift == 0 else pltpu.roll(value, shift, 0)


def rows_dot(a, b):
    return lax.dot_general(a, b, (((1,), (1,)), ((), ())), preferred_element_type=F32)


def iota(shape, axis):
    return lax.broadcasted_iota(jnp.int32, shape, axis)


def body(rows, cols, *refs):
    refs = list(refs)

    def take(count):
        head = refs[:count]
        del refs[:count]
        return head

    (b_head,) = take(1)
    small_hbm = dict(zip(SMALL, take(len(SMALL))))
    w_hbm = dict(zip(WEIGHTS, take(len(WEIGHTS))))
    (y_ref,) = take(1)
    small = dict(zip(SMALL, take(len(SMALL))))
    x_ref, w_enc1a, w_head, bias = small["x"], small["w_enc1a"], small["w_head"], small
    w_vm = dict(zip(WEIGHTS, take(len(WEIGHTS))))
    maps = dict(zip(MAPS, take(len(MAPS))))
    packs = dict(zip(SHARED, take(len(SHARED))))
    lands = dict(zip(SHARED, take(len(SHARED))))
    corner_packs = dict(zip(SHARED, take(len(SHARED))))
    corner_lands = dict(zip(SHARED, take(len(SHARED))))
    x27, w27, mb, d2, d1, acc1, acc2, y_rows = take(8)
    small_sem, w_sem, send_sem, recv_sem = take(4)

    data = lax.axis_index("data")
    row = lax.axis_index("row")
    col = lax.axis_index("col")
    go = row >= 0
    has_n, has_s, has_w, has_e = row > 0, row < rows - 1, col > 0, col < cols - 1
    has = (has_n, has_s, has_w, has_e, has_n & has_w, has_n & has_e, has_s & has_w, has_s & has_e)

    def neighbour(way):
        return (data, col + STEP[way][1], row + STEP[way][0])

    barrier = pltpu.get_barrier_semaphore()
    count = jnp.int32(0)
    for way in range(8):
        @pl.when(has[way])
        def _(way=way):
            pl.semaphore_signal(barrier, inc=1, device_id=neighbour(way), device_id_type=MESH)
        count = count + has[way].astype(jnp.int32)

    small_copy = {}
    for index, name in enumerate(SMALL):
        small_copy[name] = pltpu.make_async_copy(small_hbm[name], small[name], small_sem.at[index])
        small_copy[name].start()
    w_copy = {}
    for index, name in enumerate(WEIGHTS):
        w_copy[name] = pltpu.make_async_copy(w_hbm[name], w_vm[name], w_sem.at[index])

    def land(name, way):
        return lands[name].at[way] if way < 4 else corner_lands[name].at[way - 4]

    def pack(name, way):
        return packs[name].at[way] if way < 4 else corner_packs[name].at[way - 4]

    def copies(name, way):
        index = SHARED.index(name)
        back = OPPOSITE[way]
        return pltpu.make_async_remote_copy(
            src_ref=pack(name, way), dst_ref=land(name, back), send_sem=send_sem.at[index, way],
            recv_sem=recv_sem.at[index, back], device_id=neighbour(way), device_id_type=MESH)

    def arrival(name, way):
        index = SHARED.index(name)
        return pltpu.make_async_remote_copy(
            src_ref=pack(name, way), dst_ref=land(name, way), send_sem=send_sem.at[index, way],
            recv_sem=recv_sem.at[index, way], device_id=neighbour(way), device_id_type=MESH)

    def sublane(channels):
        return iota((16, channels), 0)

    def spot(name, way, i, j):
        side, ring, _ = MAPS[name]
        di, dj = STEP[way]
        i = i - (side - ring) if di > 0 else i
        j = j - (side - ring) if dj > 0 else j
        return i * side + j if dj == 0 else i * ring + j

    def span(side, ring, d):
        return range(side) if d == 0 else range(ring) if d < 0 else range(side - ring, side)

    def gather(name):
        side, ring, channels = MAPS[name]
        m, tiles = maps[name], tiles_of(name)
        s = sublane(channels)
        for way in range(8):
            di, dj = STEP[way]
            packed = {}
            for i in span(side, ring, di):
                for j in span(side, ring, dj):
                    e = spot(name, way, i, j)
                    value = m[ring + i, ring + j]
                    edge = 4 * (3 if di > 0 else 0) + (3 if dj > 0 else 0)
                    if way < 4:
                        t, k = e // 4, e % 4
                        value = turn(value, (4 * k if dj == 0 else k) - edge)
                        test = (s >> 2) == k if dj == 0 else (s & 3) == k
                    else:
                        t, k = 0, e
                        value = turn(value, k - edge)
                        test = s == k
                    packed[t] = value if t not in packed else jnp.where(test, value, packed[t])
            for t, value in packed.items():
                if way < 4:
                    packs[name][way, t] = value
                else:
                    corner_packs[name][way - 4] = value[0:8]

    def launch(name):
        for way in ORDER:
            @pl.when(has[way])
            def _(way=way):
                copies(name, way).start()

    def settle(names):
        for name in names:
            for way in range(8):
                @pl.when(has[way])
                def _(way=way, name=name):
                    copies(name, way).wait_send()

    def send(name):
        gather(name)
        launch(name)

    def receive(name):
        for way in range(8):
            @pl.when(has[way])
            def _(way=way):
                arrival(name, way).wait_recv()
        side, ring, channels = MAPS[name]
        m, tiles = maps[name], tiles_of(name)
        s = sublane(channels)
        zero = jnp.zeros((16, channels), BF)

        def came(way, tile):
            if way < 4:
                value = lands[name][way, tile]
            else:
                value = jnp.concatenate([corner_lands[name][way - 4], zero[0:8]], axis=0)
            return jnp.where(has[way], value, zero)

        for i in range(-ring, side + ring):
            for j in range(-ring, side + ring):
                di = -1 if i < 0 else 1 if i >= side else 0
                dj = -1 if j < 0 else 1 if j >= side else 0
                if di == 0 and dj == 0:
                    continue
                si, sj = i % side, j % side
                value = turn(m[ring + si, ring + sj], -4 * di - dj)
                hb, wb = (3 if di > 0 else 0), (3 if dj > 0 else 0)
                if di:
                    way = STEP.index((di, 0))
                    e = spot(name, OPPOSITE[way], si, sj)
                    value = jnp.where((s >> 2) == hb, turn(came(way, e // 4), 4 * hb - 4 * (e % 4) - dj), value)
                if dj:
                    way = STEP.index((0, dj))
                    e = spot(name, OPPOSITE[way], si, sj)
                    value = jnp.where((s & 3) == wb, turn(came(way, e // 4), wb - 4 * di - e % 4), value)
                if di and dj:
                    way = STEP.index((di, dj))
                    e = spot(name, OPPOSITE[way], si, sj)
                    value = jnp.where(s == 4 * hb + wb, turn(came(way, 0), 4 * hb + wb - e), value)
                m[ring + i, ring + j] = value

    def clear_outside(name):
        side, ring, channels = MAPS[name]
        m = maps[name]
        s = sublane(channels)
        zero = jnp.zeros((16, channels), BF)
        inside = [None] * 4
        for way, test in enumerate(((s >> 2) == 0, (s >> 2) == 3, (s & 3) == 0, (s & 3) == 3)):
            inside[way] = jnp.logical_or(jnp.logical_not(test), has[way])
        for i in range(-ring, side + ring):
            for j in range(-ring, side + ring):
                ways = [w for w, out in enumerate((i < 0, i >= side, j < 0, j >= side)) if out]
                if ways:
                    value = m[ring + i, ring + j]
                    for way in ways:
                        value = jnp.where(inside[way], value, zero)
                    m[ring + i, ring + j] = value

    def taps(name, out_ring):
        side, ring, channels = MAPS[name]
        m, first, size = maps[name], ring - 1 - out_ring, side + 2 * out_ring
        return [m[first + dy:first + dy + size, first + dx:first + dx + size].reshape(size * size * 16, channels)
                for dy in range(3) for dx in range(3)]

    def tap_weight(weight, t, count, first, channels, depth):
        if depth == channels:
            return w_vm[weight][pl.ds(t * depth, count * depth), :]
        parts = [w_vm[weight][pl.ds(u * depth + first, channels), :] for u in range(t, t + count)]
        return parts[0] if count == 1 else jnp.concatenate(parts, axis=0)

    def chain(values, numbers, weight, first, channels, depth):
        total, at = None, 0
        while at < len(values):
            count = 1
            if channels == 384 and weight not in TURNED:
                while count < 2 and at + count < len(values) and numbers[at + count] == numbers[at] + count:
                    count += 1
            value = values[at] if count == 1 else jnp.concatenate(values[at:at + count], axis=1)
            if weight in TURNED:
                part = rows_dot(value, w_vm[weight][pl.ds(numbers[at] * 192, 192), first:first + channels])
            else:
                part = jnp.dot(value, tap_weight(weight, numbers[at], count, first, channels, depth), preferred_element_type=F32)
            total = part if total is None else total + part
            at += count
        return total

    def conv_sum(name, weight, first, depth, out_ring=0):
        return chain(taps(name, out_ring), range(9), weight, first, MAPS[name][2], depth)

    def clear_ring(name):
        side, ring, channels = MAPS[name]
        m, wide = maps[name], side + 2 * ring
        flat, tall = jnp.zeros((ring, wide, 16, channels), BF), jnp.zeros((side, ring, 16, channels), BF)
        m[0:ring] = flat
        m[side + ring:wide] = flat
        m[ring:side + ring, 0:ring] = tall
        m[ring:side + ring, side + ring:wide] = tall

    def ring_sum(name, weight, first, depth, acc):
        side, ring, channels = MAPS[name]
        m, size = maps[name], side + 2
        lines = ((0, 1), (0, size - 1), (size - 2, size - 1))
        blank = jnp.zeros((2, 16, channels), BF)

        def product(values, numbers):
            values = [v.reshape(2 * size * 16, channels) for v in values]
            return chain(values, numbers, weight, first, channels, depth).reshape(2, size, 16, -1)

        for dy in range(3):
            out = product([jnp.concatenate([m[r + dy, dx:dx + size] for r in lines[dy]], axis=0) for dx in range(3)],
                          [3 * dy + dx for dx in range(3)])
            for n, r in enumerate(lines[dy]):
                acc[r] = acc[r] + out[n]
        for dx in range(3):
            strips = [jnp.concatenate([blank, m[2:side + 2, r + dx], blank], axis=0) for r in lines[dx]]
            out = product([jnp.concatenate([strip[dy:dy + size] for strip in strips], axis=0) for dy in range(3)],
                          [3 * dy + dx for dy in range(3)])
            for n, r in enumerate(lines[dx]):
                acc[:, r] = acc[:, r] + out[n]

    def act(total, name):
        return jnp.maximum(total + bias[name][...][None, :], 0.0).astype(BF)

    def put(name, value, out_ring=0):
        side, ring, channels = MAPS[name]
        size, first = side + 2 * out_ring, ring - out_ring
        maps[name][first:first + size, first:first + size] = value.reshape(size, size, 16, channels)

    def layer(target, source, weight, depth, out_ring=0):
        w_copy[weight].wait()

        @pl.when(go)
        def _():
            put(target, act(conv_sum(source, weight, 0, depth, out_ring), weight), out_ring)

    def pool(source, target):
        side, ring, channels = MAPS[target]
        a, b, first = maps[source], maps[target], MAPS[source][1]
        for i in range(side):
            for j in range(side):
                p, q = first + 2 * i, first + 2 * j
                b[ring + i, ring + j] = jnp.maximum(jnp.maximum(a[p, q], a[p, q + 1]), jnp.maximum(a[p + 1, q], a[p + 1, q + 1]))

    def up(value, weight, target):
        side, ring, channels = MAPS[target]
        depth = value.shape[1]
        w_copy[weight].wait()

        @pl.when(go)
        def _():
            for p in range(2):
                for q in range(2):
                    if weight in TURNED:
                        out = rows_dot(value[...], w_vm[weight][pl.ds((2 * p + q) * channels, channels), :])
                    else:
                        out = jnp.dot(value[...], w_vm[weight][pl.ds((2 * p + q) * depth, depth), :], preferred_element_type=F32)
                    out = out.astype(BF).reshape(side // 2, side // 2, 16, channels)
                    for i in range(side // 2):
                        for j in range(side // 2):
                            maps[target][ring + 2 * i + p, ring + 2 * j + q] = out[i, j]

    lane, low = iota((32, 128), 1), iota((32, 128), 0)
    for name in SMALL:
        small_copy[name].wait()
    for name in WEIGHTS:
        w_copy[name].start()
    pixels = x_ref[...].astype(F32)
    z = None
    for hb in range(4):
        pick = (((lane >> 2) & 3) == hb) & (low == 8 * (lane & 3) + (lane >> 4))
        part = jnp.dot(pixels[:, 8 * hb:8 * hb + 8, :].reshape(24, 32).astype(BF), jnp.where(pick, 1.0, 0.0).astype(BF),
                       preferred_element_type=F32)
        z = part if z is None else z + part
    spread_row, spread_lane = iota((24, 1024), 0), iota((24, 1024), 1)
    spread = ((spread_lane >> 7) == (spread_row & 7)) & ((spread_lane & 127) == (spread_row >> 3))
    z = jnp.dot(z.T.astype(BF), jnp.where(spread, 1.0, 0.0).astype(BF), preferred_element_type=F32).astype(BF)
    for hl in range(8):
        maps["x"][2 + hl, 2:10] = z[:, 128 * hl:128 * hl + 128].reshape(8, 16, 128)
    w27[...] = jnp.zeros(w27.shape, F32)
    for t in range(9):
        w27[pl.ds(3 * t, 3), :] = w_enc1a[t].astype(F32)

    pl.semaphore_wait(barrier, count)
    send("x")
    clear_ring("u1")
    clear_ring("p1")
    receive("x")

    def lanes_of(value, shift):
        return value if shift == 0 else pltpu.roll(value, shift, 1)

    for j in range(10):
        three = []
        for i in range(12):
            value = None
            for dx in range(3):
                part = lanes_of(maps["x"][i, j + dx], 3 * dx)
                value = part if value is None else value + part
            three.append(value)
        for i in range(10):
            nine = three[i] + lanes_of(three[i + 1], 9) + lanes_of(three[i + 2], 18)
            x27[i, j] = nine

    @pl.when(go)
    def _():
        put("a1", act(jnp.dot(x27[...].reshape(1600, 128), w27[...].astype(BF), preferred_element_type=F32), "enc1a"), 1)

    clear_outside("a1")
    layer("s1", "a1", "enc1b", 192)
    pool("s1", "p1")
    send("p1")
    w_copy["enc2a"].wait()

    @pl.when(go)
    def _():
        acc2[...] = conv_sum("p1", "enc2a", 0, 192, 1).reshape(acc2.shape)

    gather("s1")
    receive("p1")
    launch("s1")

    @pl.when(go)
    def _():
        ring_sum("p1", "enc2a", 0, 192, acc2)

    @pl.when(go)
    def _():
        put("a2", act(acc2[...].reshape(576, 384), "enc2a"), 1)

    clear_outside("a2")
    layer("s2", "a2", "enc2b", 384)
    pool("s2", "p2")
    send("p2")
    gather("s2")
    receive("s1")
    w_copy["dec1a"].wait()

    @pl.when(go)
    def _():
        acc1[...] = conv_sum("s1", "dec1a", 192, 384, 1).reshape(acc1.shape)

    receive("p2")
    launch("s2")
    layer("ma", "p2", "mid_a", 384, 1)
    clear_outside("ma")
    w_copy["mid_b"].wait()

    @pl.when(go)
    def _():
        mb[...] = act(conv_sum("ma", "mid_b", 0, 768), "mid_b")

    up(mb, "up2", "u2")
    send("u2")
    receive("s2")
    w_copy["dec2a"].wait()

    @pl.when(go)
    def _():
        acc2[...] = conv_sum("s2", "dec2a", 384, 768, 1).reshape(acc2.shape)

    receive("u2")

    @pl.when(go)
    def _():
        put("e2", act(conv_sum("u2", "dec2a", 0, 768, 1) + acc2[...].reshape(576, 384), "dec2a"), 1)

    clear_outside("e2")
    w_copy["dec2b"].wait()

    @pl.when(go)
    def _():
        d2[...] = act(conv_sum("e2", "dec2b", 0, 384), "dec2b")

    up(d2, "up1", "u1")
    send("u1")

    @pl.when(go)
    def _():
        acc1[...] = acc1[...] + conv_sum("u1", "dec1a", 0, 384, 1).reshape(acc1.shape)

    settle(SHARED[:-1])
    receive("u1")

    @pl.when(go)
    def _():
        ring_sum("u1", "dec1a", 0, 384, acc1)

    @pl.when(go)
    def _():
        put("e1", act(acc1[...].reshape(1600, 192), "dec1a"), 1)

    clear_outside("e1")
    w_copy["dec1b"].wait()

    @pl.when(go)
    def _():
        d1[...] = act(conv_sum("e1", "dec1b", 0, 192), "dec1b")

    @pl.when(go)
    def _():
        out_channels = y_ref.shape[0]
        for hl in range(8):
            y_rows[:, hl, :] = rows_dot(w_head[...], d1[pl.ds(128 * hl, 128), :])
        k, n = iota((128, 128), 0), iota((128, 128), 1)
        pick = ((n >> 5) == ((k >> 2) & 3)) & ((n & 31) == 8 * (k & 3) + (k >> 4))
        y = jnp.dot(y_rows[...].reshape(8 * out_channels, 128), jnp.where(pick, 1.0, 0.0), precision=lax.Precision.HIGHEST,
                    preferred_element_type=F32).reshape(out_channels, 8, 128)
        for c in range(out_channels):
            for hb in range(4):
                y_ref[c, pl.ds(8 * hb, 8), :] = y[c, :, 32 * hb:32 * hb + 32] + b_head[c]

    settle(SHARED[-1:])


def solution(mesh):
    rows = mesh.shape["row"]
    cols = mesh.shape["col"]
    tile_spec = P(("data", "row"), "col", None)

    def device_body(image, *params):
        names = ("w_enc1a", "b_enc1a", "w_enc1b", "b_enc1b", "w_enc2a", "b_enc2a", "w_enc2b", "b_enc2b", "w_mid_a", "b_mid_a",
                 "w_mid_b", "b_mid_b", "w_up2", "w_dec2a", "b_dec2a", "w_dec2b", "b_dec2b", "w_up1", "w_dec1a", "b_dec1a",
                 "w_dec1b", "b_dec1b", "w_head", "b_head")
        p = dict(zip(names, params))
        high, wide, depth = image.shape
        weights = [p["w_" + n].swapaxes(2, 3) if n in TURNED else p["w_" + n] for n in WEIGHTS]
        weights = [w.reshape(-1, w.shape[-1]) for w in weights]
        biases = [p["b_" + n] for n in BIASES]
        vmem = pl.BlockSpec(memory_space=pltpu.VMEM)
        smem = pl.BlockSpec(memory_space=pltpu.SMEM)
        hbm = pl.BlockSpec(memory_space=pl.ANY)
        out_channels = p["w_head"].shape[1]
        smalls = [image.transpose(2, 0, 1), p["w_enc1a"].reshape(9, depth, -1), p["w_head"].T] + biases
        scratch = [pltpu.VMEM(a.shape, a.dtype) for a in smalls + weights]
        scratch += [pltpu.VMEM((s + 2 * r, s + 2 * r, 16, c), BF) for s, r, c in MAPS.values()]
        scratch += [pltpu.VMEM((4, tiles_of(n), 16, MAPS[n][2]), BF) for n in SHARED] * 2
        scratch += [pltpu.VMEM((4, 8, MAPS[n][2]), BF) for n in SHARED] * 2
        scratch += [pltpu.VMEM((10, 10, 16, 128), BF), pltpu.VMEM((128, 192), F32), pltpu.VMEM((64, 768), BF),
                    pltpu.VMEM((256, 384), BF), pltpu.VMEM((1024, 192), BF), pltpu.VMEM((10, 10, 16, 192), F32),
                    pltpu.VMEM((6, 6, 16, 384), F32), pltpu.VMEM((out_channels, 8, 128), F32)]
        scratch += [pltpu.SemaphoreType.DMA((len(SMALL),)), pltpu.SemaphoreType.DMA((len(WEIGHTS),)), pltpu.SemaphoreType.DMA((len(SHARED), 8)),
                    pltpu.SemaphoreType.DMA((len(SHARED), 8))]
        y = pl.pallas_call(
            functools.partial(body, rows, cols),
            out_shape=jax.ShapeDtypeStruct((out_channels, high, wide), F32),
            in_specs=[smem] + [hbm] * (len(smalls) + len(weights)),
            out_specs=vmem,
            scratch_shapes=scratch,
            compiler_params=pltpu.CompilerParams(collective_id=0, has_side_effects=True, vmem_limit_bytes=62 * 1024 * 1024),
            name="unet",
        )(p["b_head"], *smalls, *weights)
        return y.transpose(1, 2, 0)

    def program(image, *params):
        mapped = jax.shard_map(device_body, mesh=mesh, in_specs=(tile_spec,) + tuple([P()] * len(params)), out_specs=tile_spec, check_vma=False)
        return mapped(image, *params)

    return program
```

```python
import functools

import jax
import jax.numpy as jnp
from jax import lax
from jax.experimental import pallas as pl
from jax.experimental.pallas import tpu as pltpu
from jax.sharding import PartitionSpec as P

MESH = pl.DeviceIdType.MESH
BF = jnp.bfloat16
F32 = jnp.float32
STEP = ((-1, 0), (1, 0), (0, -1), (0, 1), (-1, -1), (-1, 1), (1, -1), (1, 1))
OPPOSITE = (1, 0, 3, 2, 7, 6, 5, 4)
ORDER = (2, 3, 4, 5, 6, 7, 0, 1)
WEIGHTS = ("enc1b", "enc2a", "enc2b", "mid_a", "mid_b", "up2", "dec2a", "dec2b", "up1", "dec1a", "dec1b")
TURNED = ("up1", "dec1a")
BIASES = ("enc1a", "enc1b", "enc2a", "enc2b", "mid_a", "mid_b", "dec2a", "dec2b", "dec1a", "dec1b")
MAPS = {"x": (8, 2, 128), "s1": (8, 2, 192), "p1": (4, 2, 192), "s2": (4, 2, 384), "p2": (2, 2, 384), "u2": (4, 2, 384),
        "u1": (8, 2, 192), "a1": (8, 1, 192), "a2": (4, 1, 384), "ma": (2, 1, 768), "e2": (4, 1, 384), "e1": (8, 1, 192)}
SHARED = ("x", "s1", "p1", "s2", "p2", "u2", "u1")
SMALL = ("x", "w_enc1a", "w_head") + BIASES


def tiles_of(name):
    side, ring, _ = MAPS[name]
    return max(side * ring // 4, 1)


def turn(value, shift):
    shift = shift % 16
    return value if shift == 0 else pltpu.roll(value, shift, 0)


def rows_dot(a, b):
    return lax.dot_general(a, b, (((1,), (1,)), ((), ())), preferred_element_type=F32)


def iota(shape, axis):
    return lax.broadcasted_iota(jnp.int32, shape, axis)


def body(rows, cols, *refs):
    refs = list(refs)

    def take(count):
        head = refs[:count]
        del refs[:count]
        return head

    (b_head,) = take(1)
    small_hbm = dict(zip(SMALL, take(len(SMALL))))
    w_hbm = dict(zip(WEIGHTS, take(len(WEIGHTS))))
    (y_ref,) = take(1)
    small = dict(zip(SMALL, take(len(SMALL))))
    x_ref, w_enc1a, w_head, bias = small["x"], small["w_enc1a"], small["w_head"], small
    w_vm = dict(zip(WEIGHTS, take(len(WEIGHTS))))
    maps = dict(zip(MAPS, take(len(MAPS))))
    packs = dict(zip(SHARED, take(len(SHARED))))
    lands = dict(zip(SHARED, take(len(SHARED))))
    corner_packs = dict(zip(SHARED, take(len(SHARED))))
    corner_lands = dict(zip(SHARED, take(len(SHARED))))
    x27, w27, mb, d2, d1, acc1, acc2, acc3, y_rows = take(9)
    small_sem, w_sem, send_sem, recv_sem = take(4)

    data = lax.axis_index("data")
    row = lax.axis_index("row")
    col = lax.axis_index("col")
    go = row >= 0
    has_n, has_s, has_w, has_e = row > 0, row < rows - 1, col > 0, col < cols - 1
    has = (has_n, has_s, has_w, has_e, has_n & has_w, has_n & has_e, has_s & has_w, has_s & has_e)

    def neighbour(way):
        return (data, col + STEP[way][1], row + STEP[way][0])

    barrier = pltpu.get_barrier_semaphore()
    count = jnp.int32(0)
    for way in range(8):
        @pl.when(has[way])
        def _(way=way):
            pl.semaphore_signal(barrier, inc=1, device_id=neighbour(way), device_id_type=MESH)
        count = count + has[way].astype(jnp.int32)

    small_copy = {}
    for index, name in enumerate(SMALL):
        small_copy[name] = pltpu.make_async_copy(small_hbm[name], small[name], small_sem.at[index])
        small_copy[name].start()
    w_copy = {}
    for index, name in enumerate(WEIGHTS):
        w_copy[name] = pltpu.make_async_copy(w_hbm[name], w_vm[name], w_sem.at[index])

    def land(name, way):
        return lands[name].at[way] if way < 4 else corner_lands[name].at[way - 4]

    def pack(name, way):
        return packs[name].at[way] if way < 4 else corner_packs[name].at[way - 4]

    def copies(name, way):
        index = SHARED.index(name)
        back = OPPOSITE[way]
        return pltpu.make_async_remote_copy(
            src_ref=pack(name, way), dst_ref=land(name, back), send_sem=send_sem.at[index, way],
            recv_sem=recv_sem.at[index, back], device_id=neighbour(way), device_id_type=MESH)

    def arrival(name, way):
        index = SHARED.index(name)
        return pltpu.make_async_remote_copy(
            src_ref=pack(name, way), dst_ref=land(name, way), send_sem=send_sem.at[index, way],
            recv_sem=recv_sem.at[index, way], device_id=neighbour(way), device_id_type=MESH)

    def sublane(channels):
        return iota((16, channels), 0)

    def spot(name, way, i, j):
        side, ring, _ = MAPS[name]
        di, dj = STEP[way]
        i = i - (side - ring) if di > 0 else i
        j = j - (side - ring) if dj > 0 else j
        return i * side + j if dj == 0 else i * ring + j

    def span(side, ring, d):
        return range(side) if d == 0 else range(ring) if d < 0 else range(side - ring, side)

    def gather(name):
        side, ring, channels = MAPS[name]
        m, tiles = maps[name], tiles_of(name)
        s = sublane(channels)
        for way in range(8):
            di, dj = STEP[way]
            packed = {}
            for i in span(side, ring, di):
                for j in span(side, ring, dj):
                    e = spot(name, way, i, j)
                    value = m[ring + i, ring + j]
                    edge = 4 * (3 if di > 0 else 0) + (3 if dj > 0 else 0)
                    if way < 4:
                        t, k = e // 4, e % 4
                        value = turn(value, (4 * k if dj == 0 else k) - edge)
                        test = (s >> 2) == k if dj == 0 else (s & 3) == k
                    else:
                        t, k = 0, e
                        value = turn(value, k - edge)
                        test = s == k
                    packed[t] = value if t not in packed else jnp.where(test, value, packed[t])
            for t, value in packed.items():
                if way < 4:
                    packs[name][way, t] = value
                else:
                    corner_packs[name][way - 4] = value[0:8]

    def launch(name):
        for way in ORDER:
            @pl.when(has[way])
            def _(way=way):
                copies(name, way).start()

    def settle(names):
        for name in names:
            for way in range(8):
                @pl.when(has[way])
                def _(way=way, name=name):
                    copies(name, way).wait_send()

    def send(name):
        gather(name)
        launch(name)

    def receive(name):
        for way in range(8):
            @pl.when(has[way])
            def _(way=way):
                arrival(name, way).wait_recv()
        side, ring, channels = MAPS[name]
        m, tiles = maps[name], tiles_of(name)
        s = sublane(channels)
        zero = jnp.zeros((16, channels), BF)

        def came(way, tile):
            if way < 4:
                value = lands[name][way, tile]
            else:
                value = jnp.concatenate([corner_lands[name][way - 4], zero[0:8]], axis=0)
            return jnp.where(has[way], value, zero)

        for i in range(-ring, side + ring):
            for j in range(-ring, side + ring):
                di = -1 if i < 0 else 1 if i >= side else 0
                dj = -1 if j < 0 else 1 if j >= side else 0
                if di == 0 and dj == 0:
                    continue
                si, sj = i % side, j % side
                value = turn(m[ring + si, ring + sj], -4 * di - dj)
                hb, wb = (3 if di > 0 else 0), (3 if dj > 0 else 0)
                if di:
                    way = STEP.index((di, 0))
                    e = spot(name, OPPOSITE[way], si, sj)
                    value = jnp.where((s >> 2) == hb, turn(came(way, e // 4), 4 * hb - 4 * (e % 4) - dj), value)
                if dj:
                    way = STEP.index((0, dj))
                    e = spot(name, OPPOSITE[way], si, sj)
                    value = jnp.where((s & 3) == wb, turn(came(way, e // 4), wb - 4 * di - e % 4), value)
                if di and dj:
                    way = STEP.index((di, dj))
                    e = spot(name, OPPOSITE[way], si, sj)
                    value = jnp.where(s == 4 * hb + wb, turn(came(way, 0), 4 * hb + wb - e), value)
                m[ring + i, ring + j] = value

    def clear_outside(name):
        side, ring, channels = MAPS[name]
        m = maps[name]
        s = sublane(channels)
        zero = jnp.zeros((16, channels), BF)
        inside = [None] * 4
        for way, test in enumerate(((s >> 2) == 0, (s >> 2) == 3, (s & 3) == 0, (s & 3) == 3)):
            inside[way] = jnp.logical_or(jnp.logical_not(test), has[way])
        for i in range(-ring, side + ring):
            for j in range(-ring, side + ring):
                ways = [w for w, out in enumerate((i < 0, i >= side, j < 0, j >= side)) if out]
                if ways:
                    value = m[ring + i, ring + j]
                    for way in ways:
                        value = jnp.where(inside[way], value, zero)
                    m[ring + i, ring + j] = value

    def taps(name, out_ring):
        side, ring, channels = MAPS[name]
        m, first, size = maps[name], ring - 1 - out_ring, side + 2 * out_ring
        return [m[first + dy:first + dy + size, first + dx:first + dx + size].reshape(size * size * 16, channels)
                for dy in range(3) for dx in range(3)]

    def tap_weight(weight, t, count, first, channels, depth):
        if depth == channels:
            return w_vm[weight][pl.ds(t * depth, count * depth), :]
        parts = [w_vm[weight][pl.ds(u * depth + first, channels), :] for u in range(t, t + count)]
        return parts[0] if count == 1 else jnp.concatenate(parts, axis=0)

    def chain(values, numbers, weight, first, channels, depth):
        total, at = None, 0
        while at < len(values):
            count = 1
            if channels == 384 and weight not in TURNED:
                while count < 2 and at + count < len(values) and numbers[at + count] == numbers[at] + count:
                    count += 1
            value = values[at] if count == 1 else jnp.concatenate(values[at:at + count], axis=1)
            if weight in TURNED:
                part = rows_dot(value, w_vm[weight][pl.ds(numbers[at] * 192, 192), first:first + channels])
            else:
                part = jnp.dot(value, tap_weight(weight, numbers[at], count, first, channels, depth), preferred_element_type=F32)
            total = part if total is None else total + part
            at += count
        return total

    def conv_sum(name, weight, first, depth, out_ring=0, some=range(9)):
        values = taps(name, out_ring)
        return chain([values[t] for t in some], some, weight, first, MAPS[name][2], depth)

    def clear_ring(name):
        side, ring, channels = MAPS[name]
        m, wide = maps[name], side + 2 * ring
        flat, tall = jnp.zeros((ring, wide, 16, channels), BF), jnp.zeros((side, ring, 16, channels), BF)
        m[0:ring] = flat
        m[side + ring:wide] = flat
        m[ring:side + ring, 0:ring] = tall
        m[ring:side + ring, side + ring:wide] = tall

    def ring_sum(name, weight, first, depth, acc, side=None):
        channels = MAPS[name][2]
        side = MAPS[name][0] if side is None else side
        m, size = maps[name], side + 2
        lines = ((0, 1), (0, size - 1), (size - 2, size - 1))
        blank = jnp.zeros((2, 16, channels), BF)

        def product(values, numbers):
            values = [v.reshape(2 * size * 16, channels) for v in values]
            return chain(values, numbers, weight, first, channels, depth).reshape(2, size, 16, -1)

        for dy in range(3):
            out = product([jnp.concatenate([m[r + dy, dx:dx + size] for r in lines[dy]], axis=0) for dx in range(3)],
                          [3 * dy + dx for dx in range(3)])
            for n, r in enumerate(lines[dy]):
                acc[r] = acc[r] + out[n]
        for dx in range(3):
            strips = [jnp.concatenate([blank, m[2:side + 2, r + dx], blank], axis=0) for r in lines[dx]]
            out = product([jnp.concatenate([strip[dy:dy + size] for strip in strips], axis=0) for dy in range(3)],
                          [3 * dy + dx for dy in range(3)])
            for n, r in enumerate(lines[dx]):
                acc[:, r] = acc[:, r] + out[n]

    def act(total, name):
        return jnp.maximum(total + bias[name][...][None, :], 0.0).astype(BF)

    def put(name, value, out_ring=0):
        side, ring, channels = MAPS[name]
        size, first = side + 2 * out_ring, ring - out_ring
        maps[name][first:first + size, first:first + size] = value.reshape(size, size, 16, channels)

    def layer(target, source, weight, depth, out_ring=0, after=None):
        w_copy[weight].wait()

        @pl.when(go)
        def _():
            put(target, act(conv_sum(source, weight, 0, depth, out_ring), weight), out_ring)
            after()

    def pool(source, target):
        side, ring, channels = MAPS[target]
        a, b, first = maps[source], maps[target], MAPS[source][1]
        for i in range(side):
            for j in range(side):
                p, q = first + 2 * i, first + 2 * j
                b[ring + i, ring + j] = jnp.maximum(jnp.maximum(a[p, q], a[p, q + 1]), jnp.maximum(a[p + 1, q], a[p + 1, q + 1]))

    def up(value, weight, target):
        side, ring, channels = MAPS[target]
        depth = value.shape[1]
        w_copy[weight].wait()

        @pl.when(go)
        def _():
            for p in range(2):
                for q in range(2):
                    if weight in TURNED:
                        out = rows_dot(value[...], w_vm[weight][pl.ds((2 * p + q) * channels, channels), :])
                    else:
                        out = jnp.dot(value[...], w_vm[weight][pl.ds((2 * p + q) * depth, depth), :], preferred_element_type=F32)
                    out = out.astype(BF).reshape(side // 2, side // 2, 16, channels)
                    for i in range(side // 2):
                        for j in range(side // 2):
                            maps[target][ring + 2 * i + p, ring + 2 * j + q] = out[i, j]
            gather(target)

    lane, low = iota((32, 128), 1), iota((32, 128), 0)
    for name in SMALL:
        small_copy[name].wait()
    for name in WEIGHTS:
        w_copy[name].start()
    pixels = x_ref[...].astype(F32)
    z = None
    for hb in range(4):
        pick = (((lane >> 2) & 3) == hb) & (low == 8 * (lane & 3) + (lane >> 4))
        part = jnp.dot(pixels[:, 8 * hb:8 * hb + 8, :].reshape(24, 32).astype(BF), jnp.where(pick, 1.0, 0.0).astype(BF),
                       preferred_element_type=F32)
        z = part if z is None else z + part
    spread_row, spread_lane = iota((24, 1024), 0), iota((24, 1024), 1)
    spread = ((spread_lane >> 7) == (spread_row & 7)) & ((spread_lane & 127) == (spread_row >> 3))
    z = jnp.dot(z.T.astype(BF), jnp.where(spread, 1.0, 0.0).astype(BF), preferred_element_type=F32).astype(BF)
    for hl in range(8):
        maps["x"][2 + hl, 2:10] = z[:, 128 * hl:128 * hl + 128].reshape(8, 16, 128)
    w27[...] = jnp.zeros(w27.shape, F32)
    for t in range(9):
        w27[pl.ds(3 * t, 3), :] = w_enc1a[t].astype(F32)

    pl.semaphore_wait(barrier, count)
    def lanes_of(value, shift):
        return value if shift == 0 else pltpu.roll(value, shift, 1)

    def patches(columns, lines):
        for j in columns:
            three = {}
            for i in sorted({i + d for i in lines for d in range(3)}):
                value = None
                for dx in range(3):
                    part = lanes_of(maps["x"][i, j + dx], 3 * dx)
                    value = part if value is None else value + part
                three[i] = value
            for i in lines:
                x27[i, j] = three[i] + lanes_of(three[i + 1], 9) + lanes_of(three[i + 2], 18)

    def enc1a(value):
        return act(jnp.dot(value.reshape(-1, 128), w27[...].astype(BF), preferred_element_type=F32), "enc1a").reshape(-1, 16, 192)

    send("x")
    patches(range(2, 8), range(2, 8))
    clear_ring("u1")
    clear_ring("p1")
    a1 = maps["a1"]
    a1[0:2] = jnp.zeros((2, 10, 16, 192), BF)
    a1[8:10] = jnp.zeros((2, 10, 16, 192), BF)
    a1[2:8, 0:2] = jnp.zeros((6, 2, 16, 192), BF)
    a1[2:8, 8:10] = jnp.zeros((6, 2, 16, 192), BF)

    @pl.when(go)
    def _():
        a1[2:8, 2:8] = enc1a(x27[2:8, 2:8]).reshape(6, 6, 16, 192)

    w_copy["enc1b"].wait()

    @pl.when(go)
    def _():
        acc3[...] = conv_sum("a1", "enc1b", 0, 192).reshape(acc3.shape)

    receive("x")
    patches(range(2, 8), (0, 1, 8, 9))
    patches((0, 1, 8, 9), range(10))

    @pl.when(go)
    def _():
        out = enc1a(jnp.concatenate([x27[0:2].reshape(20, 16, 128), x27[8:10].reshape(20, 16, 128),
                                     x27[2:8, 0:2].reshape(12, 16, 128), x27[2:8, 8:10].reshape(12, 16, 128)], axis=0))
        a1[0:2] = out[0:20].reshape(2, 10, 16, 192)
        a1[8:10] = out[20:40].reshape(2, 10, 16, 192)
        a1[2:8, 0:2] = out[40:52].reshape(6, 2, 16, 192)
        a1[2:8, 8:10] = out[52:64].reshape(6, 2, 16, 192)
        clear_outside("a1")

    @pl.when(go)
    def _():
        ring_sum("a1", "enc1b", 0, 192, acc3, 6)
        put("s1", act(acc3[...].reshape(1024, 192), "enc1b"))
        pool("s1", "p1")
        gather("p1")

    launch("p1")
    w_copy["enc2a"].wait()

    @pl.when(go)
    def _():
        acc2[...] = conv_sum("p1", "enc2a", 0, 192, 1).reshape(acc2.shape)

    gather("s1")
    receive("p1")
    launch("s1")

    @pl.when(go)
    def _():
        ring_sum("p1", "enc2a", 0, 192, acc2)
        put("a2", act(acc2[...].reshape(576, 384), "enc2a"), 1)
        clear_outside("a2")


    def halve():
        pool("s2", "p2")
        gather("p2")

    layer("s2", "a2", "enc2b", 384, 0, halve)
    launch("p2")
    gather("s2")
    receive("s1")
    w_copy["dec1a"].wait()

    @pl.when(go)
    def _():
        acc1[...] = conv_sum("s1", "dec1a", 192, 384, 1, range(6)).reshape(acc1.shape)

    receive("p2")
    launch("s2")
    layer("ma", "p2", "mid_a", 384, 1, lambda: clear_outside("ma"))
    w_copy["mid_b"].wait()

    @pl.when(go)
    def _():
        mb[...] = act(conv_sum("ma", "mid_b", 0, 768), "mid_b")

    up(mb, "up2", "u2")
    launch("u2")
    receive("s2")
    w_copy["dec2a"].wait()

    @pl.when(go)
    def _():
        acc2[...] = conv_sum("s2", "dec2a", 384, 768, 1).reshape(acc2.shape)

    receive("u2")

    @pl.when(go)
    def _():
        put("e2", act(conv_sum("u2", "dec2a", 0, 768, 1) + acc2[...].reshape(576, 384), "dec2a"), 1)
        clear_outside("e2")

    w_copy["dec2b"].wait()

    @pl.when(go)
    def _():
        d2[...] = act(conv_sum("e2", "dec2b", 0, 384), "dec2b")

    up(d2, "up1", "u1")
    launch("u1")

    @pl.when(go)
    def _():
        late = conv_sum("u1", "dec1a", 0, 384, 1) + conv_sum("s1", "dec1a", 192, 384, 1, range(6, 9))
        acc1[...] = acc1[...] + late.reshape(acc1.shape)

    settle(SHARED[:-1])
    receive("u1")

    @pl.when(go)
    def _():
        ring_sum("u1", "dec1a", 0, 384, acc1)
        put("e1", act(acc1[...].reshape(1600, 192), "dec1a"), 1)
        clear_outside("e1")

    w_copy["dec1b"].wait()

    @pl.when(go)
    def _():
        d1[...] = act(conv_sum("e1", "dec1b", 0, 192), "dec1b")

    @pl.when(go)
    def _():
        out_channels = y_ref.shape[0]
        for hl in range(8):
            y_rows[:, hl, :] = rows_dot(w_head[...], d1[pl.ds(128 * hl, 128), :])
        k, n = iota((128, 128), 0), iota((128, 128), 1)
        pick = ((n >> 5) == ((k >> 2) & 3)) & ((n & 31) == 8 * (k & 3) + (k >> 4))
        y = jnp.dot(y_rows[...].reshape(8 * out_channels, 128), jnp.where(pick, 1.0, 0.0), precision=lax.Precision.HIGHEST,
                    preferred_element_type=F32).reshape(out_channels, 8, 128)
        for c in range(out_channels):
            for hb in range(4):
                y_ref[c, pl.ds(8 * hb, 8), :] = y[c, :, 32 * hb:32 * hb + 32] + b_head[c]

    settle(SHARED[-1:])


def solution(mesh):
    rows = mesh.shape["row"]
    cols = mesh.shape["col"]
    tile_spec = P(("data", "row"), "col", None)

    def device_body(image, *params):
        names = ("w_enc1a", "b_enc1a", "w_enc1b", "b_enc1b", "w_enc2a", "b_enc2a", "w_enc2b", "b_enc2b", "w_mid_a", "b_mid_a",
                 "w_mid_b", "b_mid_b", "w_up2", "w_dec2a", "b_dec2a", "w_dec2b", "b_dec2b", "w_up1", "w_dec1a", "b_dec1a",
                 "w_dec1b", "b_dec1b", "w_head", "b_head")
        p = dict(zip(names, params))
        high, wide, depth = image.shape
        weights = [p["w_" + n].swapaxes(2, 3) if n in TURNED else p["w_" + n] for n in WEIGHTS]
        weights = [w.reshape(-1, w.shape[-1]) for w in weights]
        biases = [p["b_" + n] for n in BIASES]
        vmem = pl.BlockSpec(memory_space=pltpu.VMEM)
        smem = pl.BlockSpec(memory_space=pltpu.SMEM)
        hbm = pl.BlockSpec(memory_space=pl.ANY)
        out_channels = p["w_head"].shape[1]
        smalls = [image.transpose(2, 0, 1), p["w_enc1a"].reshape(9, depth, -1), p["w_head"].T] + biases
        scratch = [pltpu.VMEM(a.shape, a.dtype) for a in smalls + weights]
        scratch += [pltpu.VMEM((s + 2 * r, s + 2 * r, 16, c), BF) for s, r, c in MAPS.values()]
        scratch += [pltpu.VMEM((4, tiles_of(n), 16, MAPS[n][2]), BF) for n in SHARED] * 2
        scratch += [pltpu.VMEM((4, 8, MAPS[n][2]), BF) for n in SHARED] * 2
        scratch += [pltpu.VMEM((10, 10, 16, 128), BF), pltpu.VMEM((128, 192), F32), pltpu.VMEM((64, 768), BF),
                    pltpu.VMEM((256, 384), BF), pltpu.VMEM((1024, 192), BF), pltpu.VMEM((10, 10, 16, 192), F32),
                    pltpu.VMEM((6, 6, 16, 384), F32), pltpu.VMEM((8, 8, 16, 192), F32), pltpu.VMEM((out_channels, 8, 128), F32)]
        scratch += [pltpu.SemaphoreType.DMA((len(SMALL),)), pltpu.SemaphoreType.DMA((len(WEIGHTS),)), pltpu.SemaphoreType.DMA((len(SHARED), 8)),
                    pltpu.SemaphoreType.DMA((len(SHARED), 8))]
        y = pl.pallas_call(
            functools.partial(body, rows, cols),
            out_shape=jax.ShapeDtypeStruct((out_channels, high, wide), F32),
            in_specs=[smem] + [hbm] * (len(smalls) + len(weights)),
            out_specs=vmem,
            scratch_shapes=scratch,
            compiler_params=pltpu.CompilerParams(collective_id=0, has_side_effects=True, vmem_limit_bytes=62 * 1024 * 1024),
            name="unet",
        )(p["b_head"], *smalls, *weights)
        return y.transpose(1, 2, 0)

    def program(image, *params):
        mapped = jax.shard_map(device_body, mesh=mesh, in_specs=(tile_spec,) + tuple([P()] * len(params)), out_specs=tile_spec, check_vma=False)
        return mapped(image, *params)

    return program
```

```python
import functools

import jax
import jax.numpy as jnp
from jax import lax
from jax.experimental import pallas as pl
from jax.experimental.pallas import tpu as pltpu
from jax.sharding import PartitionSpec as P

MESH = pl.DeviceIdType.MESH
BF = jnp.bfloat16
F32 = jnp.float32
STEP = ((-1, 0), (1, 0), (0, -1), (0, 1), (-1, -1), (-1, 1), (1, -1), (1, 1))
OPPOSITE = (1, 0, 3, 2, 7, 6, 5, 4)
ORDER = (2, 3, 4, 5, 6, 7, 0, 1)
WEIGHTS = ("enc1b", "enc2a", "enc2b", "mid_a", "mid_b", "up2", "dec2a", "dec2b", "up1", "dec1a", "dec1b")
TURNED = ("up1", "dec1a")
BIASES = ("enc1a", "enc1b", "enc2a", "enc2b", "mid_a", "mid_b", "dec2a", "dec2b", "dec1a", "dec1b")
MAPS = {"x": (8, 2, 128), "s1": (8, 2, 192), "p1": (4, 2, 192), "s2": (4, 2, 384), "p2": (2, 2, 384), "u2": (4, 2, 384),
        "u1": (8, 2, 192), "a1": (8, 1, 192), "a2": (4, 1, 384), "ma": (2, 1, 768), "e2": (4, 1, 384), "e1": (8, 1, 192)}
SHARED = ("x", "s1", "p1", "s2", "p2", "u2", "u1")
SMALL = ("x", "w_enc1a", "w_head") + BIASES


def tiles_of(name):
    side, ring, _ = MAPS[name]
    return max(side * ring // 4, 1)


def turn(value, shift):
    shift = shift % 16
    return value if shift == 0 else pltpu.roll(value, shift, 0)


def rows_dot(a, b):
    return lax.dot_general(a, b, (((1,), (1,)), ((), ())), preferred_element_type=F32)


def iota(shape, axis):
    return lax.broadcasted_iota(jnp.int32, shape, axis)


def body(rows, cols, *refs):
    refs = list(refs)

    def take(count):
        head = refs[:count]
        del refs[:count]
        return head

    (b_head,) = take(1)
    small_hbm = dict(zip(SMALL, take(len(SMALL))))
    w_hbm = dict(zip(WEIGHTS, take(len(WEIGHTS))))
    (y_ref,) = take(1)
    small = dict(zip(SMALL, take(len(SMALL))))
    x_ref, w_enc1a, w_head, bias = small["x"], small["w_enc1a"], small["w_head"], small
    w_vm = dict(zip(WEIGHTS, take(len(WEIGHTS))))
    maps = dict(zip(MAPS, take(len(MAPS))))
    packs = dict(zip(SHARED, take(len(SHARED))))
    lands = dict(zip(SHARED, take(len(SHARED))))
    corner_packs = dict(zip(SHARED, take(len(SHARED))))
    corner_lands = dict(zip(SHARED, take(len(SHARED))))
    x27, w27, mb, d2, d1, acc1, acc2, acc3, y_rows = take(9)
    small_sem, w_sem, send_sem, recv_sem = take(4)

    data = lax.axis_index("data")
    row = lax.axis_index("row")
    col = lax.axis_index("col")
    go = row >= 0
    has_n, has_s, has_w, has_e = row > 0, row < rows - 1, col > 0, col < cols - 1
    has = (has_n, has_s, has_w, has_e, has_n & has_w, has_n & has_e, has_s & has_w, has_s & has_e)

    def neighbour(way):
        return (data, col + STEP[way][1], row + STEP[way][0])

    barrier = pltpu.get_barrier_semaphore()
    count = jnp.int32(0)
    for way in range(8):
        @pl.when(has[way])
        def _(way=way):
            pl.semaphore_signal(barrier, inc=1, device_id=neighbour(way), device_id_type=MESH)
        count = count + has[way].astype(jnp.int32)

    small_copy = {}
    for index, name in enumerate(SMALL):
        small_copy[name] = pltpu.make_async_copy(small_hbm[name], small[name], small_sem.at[index])
        small_copy[name].start()
    w_copy = {}
    for index, name in enumerate(WEIGHTS):
        w_copy[name] = pltpu.make_async_copy(w_hbm[name], w_vm[name], w_sem.at[index])

    def land(name, way):
        return lands[name].at[way] if way < 4 else corner_lands[name].at[way - 4]

    def pack(name, way):
        return packs[name].at[way] if way < 4 else corner_packs[name].at[way - 4]

    def copies(name, way):
        index = SHARED.index(name)
        back = OPPOSITE[way]
        return pltpu.make_async_remote_copy(
            src_ref=pack(name, way), dst_ref=land(name, back), send_sem=send_sem.at[index, way],
            recv_sem=recv_sem.at[index, back], device_id=neighbour(way), device_id_type=MESH)

    def arrival(name, way):
        index = SHARED.index(name)
        return pltpu.make_async_remote_copy(
            src_ref=pack(name, way), dst_ref=land(name, way), send_sem=send_sem.at[index, way],
            recv_sem=recv_sem.at[index, way], device_id=neighbour(way), device_id_type=MESH)

    def sublane(channels):
        return iota((16, channels), 0)

    def spot(name, way, i, j):
        side, ring, _ = MAPS[name]
        di, dj = STEP[way]
        i = i - (side - ring) if di > 0 else i
        j = j - (side - ring) if dj > 0 else j
        return i * side + j if dj == 0 else i * ring + j

    def span(side, ring, d):
        return range(side) if d == 0 else range(ring) if d < 0 else range(side - ring, side)

    def gather(name):
        side, ring, channels = MAPS[name]
        m, tiles = maps[name], tiles_of(name)
        s = sublane(channels)
        for way in range(8):
            di, dj = STEP[way]
            packed = {}
            for i in span(side, ring, di):
                for j in span(side, ring, dj):
                    e = spot(name, way, i, j)
                    value = m[ring + i, ring + j]
                    edge = 4 * (3 if di > 0 else 0) + (3 if dj > 0 else 0)
                    if way < 4:
                        t, k = e // 4, e % 4
                        value = turn(value, (4 * k if dj == 0 else k) - edge)
                        test = (s >> 2) == k if dj == 0 else (s & 3) == k
                    else:
                        t, k = 0, e
                        value = turn(value, k - edge)
                        test = s == k
                    packed[t] = value if t not in packed else jnp.where(test, value, packed[t])
            for t, value in packed.items():
                if way < 4:
                    packs[name][way, t] = value
                else:
                    corner_packs[name][way - 4] = value[0:8]

    def launch(name):
        for way in ORDER:
            @pl.when(has[way])
            def _(way=way):
                copies(name, way).start()

    def settle(names):
        for name in names:
            for way in range(8):
                @pl.when(has[way])
                def _(way=way, name=name):
                    copies(name, way).wait_send()

    def send(name):
        gather(name)
        launch(name)

    def receive(name):
        for way in range(8):
            @pl.when(has[way])
            def _(way=way):
                arrival(name, way).wait_recv()
        side, ring, channels = MAPS[name]
        m, tiles = maps[name], tiles_of(name)
        s = sublane(channels)
        zero = jnp.zeros((16, channels), BF)

        def came(way, tile):
            if way < 4:
                value = lands[name][way, tile]
            else:
                value = jnp.concatenate([corner_lands[name][way - 4], zero[0:8]], axis=0)
            return jnp.where(has[way], value, zero)

        for i in range(-ring, side + ring):
            for j in range(-ring, side + ring):
                di = -1 if i < 0 else 1 if i >= side else 0
                dj = -1 if j < 0 else 1 if j >= side else 0
                if di == 0 and dj == 0:
                    continue
                si, sj = i % side, j % side
                value = turn(m[ring + si, ring + sj], -4 * di - dj)
                hb, wb = (3 if di > 0 else 0), (3 if dj > 0 else 0)
                if di:
                    way = STEP.index((di, 0))
                    e = spot(name, OPPOSITE[way], si, sj)
                    value = jnp.where((s >> 2) == hb, turn(came(way, e // 4), 4 * hb - 4 * (e % 4) - dj), value)
                if dj:
                    way = STEP.index((0, dj))
                    e = spot(name, OPPOSITE[way], si, sj)
                    value = jnp.where((s & 3) == wb, turn(came(way, e // 4), wb - 4 * di - e % 4), value)
                if di and dj:
                    way = STEP.index((di, dj))
                    e = spot(name, OPPOSITE[way], si, sj)
                    value = jnp.where(s == 4 * hb + wb, turn(came(way, 0), 4 * hb + wb - e), value)
                m[ring + i, ring + j] = value

    def clear_outside(name):
        side, ring, channels = MAPS[name]
        m = maps[name]
        s = sublane(channels)
        zero = jnp.zeros((16, channels), BF)
        inside = [None] * 4
        for way, test in enumerate(((s >> 2) == 0, (s >> 2) == 3, (s & 3) == 0, (s & 3) == 3)):
            inside[way] = jnp.logical_or(jnp.logical_not(test), has[way])
        for i in range(-ring, side + ring):
            for j in range(-ring, side + ring):
                ways = [w for w, out in enumerate((i < 0, i >= side, j < 0, j >= side)) if out]
                if ways:
                    value = m[ring + i, ring + j]
                    for way in ways:
                        value = jnp.where(inside[way], value, zero)
                    m[ring + i, ring + j] = value

    def taps(name, out_ring):
        side, ring, channels = MAPS[name]
        m, first, size = maps[name], ring - 1 - out_ring, side + 2 * out_ring
        return [m[first + dy:first + dy + size, first + dx:first + dx + size].reshape(size * size * 16, channels)
                for dy in range(3) for dx in range(3)]

    def tap_weight(weight, t, count, first, channels, depth):
        if depth == channels:
            return w_vm[weight][pl.ds(t * depth, count * depth), :]
        parts = [w_vm[weight][pl.ds(u * depth + first, channels), :] for u in range(t, t + count)]
        return parts[0] if count == 1 else jnp.concatenate(parts, axis=0)

    def chain(values, numbers, weight, first, channels, depth):
        total, at = None, 0
        while at < len(values):
            count = 1
            if channels == 384 and weight not in TURNED:
                while count < 2 and at + count < len(values) and numbers[at + count] == numbers[at] + count:
                    count += 1
            value = values[at] if count == 1 else jnp.concatenate(values[at:at + count], axis=1)
            if weight in TURNED:
                part = rows_dot(value, w_vm[weight][pl.ds(numbers[at] * 192, 192), first:first + channels])
            else:
                part = jnp.dot(value, tap_weight(weight, numbers[at], count, first, channels, depth), preferred_element_type=F32)
            total = part if total is None else total + part
            at += count
        return total

    def conv_sum(name, weight, first, depth, out_ring=0, some=range(9)):
        values = taps(name, out_ring)
        return chain([values[t] for t in some], some, weight, first, MAPS[name][2], depth)

    def clear_ring(name):
        side, ring, channels = MAPS[name]
        m, wide = maps[name], side + 2 * ring
        flat, tall = jnp.zeros((ring, wide, 16, channels), BF), jnp.zeros((side, ring, 16, channels), BF)
        m[0:ring] = flat
        m[side + ring:wide] = flat
        m[ring:side + ring, 0:ring] = tall
        m[ring:side + ring, side + ring:wide] = tall

    def ring_sum(name, weight, first, depth, acc, side=None):
        channels = MAPS[name][2]
        side = MAPS[name][0] if side is None else side
        m, size = maps[name], side + 2
        lines = ((0, 1), (0, size - 1), (size - 2, size - 1))
        blank = jnp.zeros((2, 16, channels), BF)

        def product(values, numbers):
            values = [v.reshape(2 * size * 16, channels) for v in values]
            return chain(values, numbers, weight, first, channels, depth).reshape(2, size, 16, -1)

        for dy in range(3):
            out = product([jnp.concatenate([m[r + dy, dx:dx + size] for r in lines[dy]], axis=0) for dx in range(3)],
                          [3 * dy + dx for dx in range(3)])
            for n, r in enumerate(lines[dy]):
                acc[r] = acc[r] + out[n]
        for dx in range(3):
            strips = [jnp.concatenate([blank, m[2:side + 2, r + dx], blank], axis=0) for r in lines[dx]]
            out = product([jnp.concatenate([strip[dy:dy + size] for strip in strips], axis=0) for dy in range(3)],
                          [3 * dy + dx for dy in range(3)])
            for n, r in enumerate(lines[dx]):
                acc[:, r] = acc[:, r] + out[n]

    def act(total, name):
        return jnp.maximum(total + bias[name][...][None, :], 0.0).astype(BF)

    def put(name, value, out_ring=0):
        side, ring, channels = MAPS[name]
        size, first = side + 2 * out_ring, ring - out_ring
        maps[name][first:first + size, first:first + size] = value.reshape(size, size, 16, channels)

    def layer(target, source, weight, depth, out_ring=0, after=None):
        w_copy[weight].wait()

        @pl.when(go)
        def _():
            put(target, act(conv_sum(source, weight, 0, depth, out_ring), weight), out_ring)
            after()

    def pool(source, target):
        side, ring, channels = MAPS[target]
        a, b, first = maps[source], maps[target], MAPS[source][1]
        for i in range(side):
            for j in range(side):
                p, q = first + 2 * i, first + 2 * j
                b[ring + i, ring + j] = jnp.maximum(jnp.maximum(a[p, q], a[p, q + 1]), jnp.maximum(a[p + 1, q], a[p + 1, q + 1]))

    def up(value, weight, target):
        side, ring, channels = MAPS[target]
        depth = value.shape[1]
        w_copy[weight].wait()

        @pl.when(go)
        def _():
            for p in range(2):
                for q in range(2):
                    if weight in TURNED:
                        out = rows_dot(value[...], w_vm[weight][pl.ds((2 * p + q) * channels, channels), :])
                    else:
                        out = jnp.dot(value[...], w_vm[weight][pl.ds((2 * p + q) * depth, depth), :], preferred_element_type=F32)
                    out = out.astype(BF).reshape(side // 2, side // 2, 16, channels)
                    for i in range(side // 2):
                        for j in range(side // 2):
                            maps[target][ring + 2 * i + p, ring + 2 * j + q] = out[i, j]
            gather(target)

    lane, low = iota((32, 128), 1), iota((32, 128), 0)
    for name in SMALL:
        small_copy[name].wait()
    for name in WEIGHTS:
        w_copy[name].start()
    pixels = x_ref[...].astype(F32)
    z = None
    for hb in range(4):
        pick = (((lane >> 2) & 3) == hb) & (low == 8 * (lane & 3) + (lane >> 4))
        part = jnp.dot(pixels[:, 8 * hb:8 * hb + 8, :].reshape(24, 32).astype(BF), jnp.where(pick, 1.0, 0.0).astype(BF),
                       preferred_element_type=F32)
        z = part if z is None else z + part
    spread_row, spread_lane = iota((24, 1024), 0), iota((24, 1024), 1)
    spread = ((spread_lane >> 7) == (spread_row & 7)) & ((spread_lane & 127) == (spread_row >> 3))
    z = jnp.dot(z.T.astype(BF), jnp.where(spread, 1.0, 0.0).astype(BF), preferred_element_type=F32).astype(BF)
    for hl in range(8):
        maps["x"][2 + hl, 2:10] = z[:, 128 * hl:128 * hl + 128].reshape(8, 16, 128)

    pl.semaphore_wait(barrier, count)
    def lanes_of(value, shift):
        return value if shift == 0 else pltpu.roll(value, shift, 1)

    def patches(columns, lines):
        for j in columns:
            three = {}
            for i in sorted({i + d for i in lines for d in range(3)}):
                value = None
                for dx in range(3):
                    part = lanes_of(maps["x"][i, j + dx], 3 * dx)
                    value = part if value is None else value + part
                three[i] = value
            for i in lines:
                x27[i, j] = three[i] + lanes_of(three[i + 1], 9) + lanes_of(three[i + 2], 18)

    def enc1a(value):
        return act(jnp.dot(value.reshape(-1, 128), w27[...].astype(BF), preferred_element_type=F32), "enc1a").reshape(-1, 16, 192)

    send("x")
    w27[...] = jnp.zeros(w27.shape, F32)
    for t in range(9):
        w27[pl.ds(3 * t, 3), :] = w_enc1a[t].astype(F32)
    patches(range(2, 8), range(2, 8))
    clear_ring("u1")
    clear_ring("p1")
    a1 = maps["a1"]
    a1[0:2] = jnp.zeros((2, 10, 16, 192), BF)
    a1[8:10] = jnp.zeros((2, 10, 16, 192), BF)
    a1[2:8, 0:2] = jnp.zeros((6, 2, 16, 192), BF)
    a1[2:8, 8:10] = jnp.zeros((6, 2, 16, 192), BF)

    @pl.when(go)
    def _():
        a1[2:8, 2:8] = enc1a(x27[2:8, 2:8]).reshape(6, 6, 16, 192)

    w_copy["enc1b"].wait()

    @pl.when(go)
    def _():
        acc3[...] = conv_sum("a1", "enc1b", 0, 192).reshape(acc3.shape)

    receive("x")
    patches(range(2, 8), (0, 1, 8, 9))
    patches((0, 1, 8, 9), range(10))

    @pl.when(go)
    def _():
        out = enc1a(jnp.concatenate([x27[0:2].reshape(20, 16, 128), x27[8:10].reshape(20, 16, 128),
                                     x27[2:8, 0:2].reshape(12, 16, 128), x27[2:8, 8:10].reshape(12, 16, 128)], axis=0))
        a1[0:2] = out[0:20].reshape(2, 10, 16, 192)
        a1[8:10] = out[20:40].reshape(2, 10, 16, 192)
        a1[2:8, 0:2] = out[40:52].reshape(6, 2, 16, 192)
        a1[2:8, 8:10] = out[52:64].reshape(6, 2, 16, 192)
        clear_outside("a1")

    @pl.when(go)
    def _():
        ring_sum("a1", "enc1b", 0, 192, acc3, 6)
        put("s1", act(acc3[...].reshape(1024, 192), "enc1b"))
        pool("s1", "p1")
        gather("p1")

    launch("p1")
    w_copy["enc2a"].wait()

    @pl.when(go)
    def _():
        acc2[...] = conv_sum("p1", "enc2a", 0, 192, 1).reshape(acc2.shape)

    gather("s1")
    receive("p1")
    launch("s1")

    @pl.when(go)
    def _():
        ring_sum("p1", "enc2a", 0, 192, acc2)
        put("a2", act(acc2[...].reshape(576, 384), "enc2a"), 1)
        clear_outside("a2")


    def halve():
        pool("s2", "p2")
        gather("p2")

    layer("s2", "a2", "enc2b", 384, 0, halve)
    launch("p2")
    gather("s2")
    receive("s1")
    w_copy["dec1a"].wait()

    @pl.when(go)
    def _():
        acc1[...] = conv_sum("s1", "dec1a", 192, 384, 1, range(7)).reshape(acc1.shape)

    receive("p2")
    launch("s2")
    layer("ma", "p2", "mid_a", 384, 1, lambda: clear_outside("ma"))
    w_copy["mid_b"].wait()

    @pl.when(go)
    def _():
        mb[...] = act(conv_sum("ma", "mid_b", 0, 768), "mid_b")

    up(mb, "up2", "u2")
    launch("u2")
    receive("s2")
    w_copy["dec2a"].wait()

    @pl.when(go)
    def _():
        acc2[...] = conv_sum("s2", "dec2a", 384, 768, 1).reshape(acc2.shape)

    receive("u2")

    @pl.when(go)
    def _():
        put("e2", act(conv_sum("u2", "dec2a", 0, 768, 1) + acc2[...].reshape(576, 384), "dec2a"), 1)
        clear_outside("e2")

    w_copy["dec2b"].wait()

    @pl.when(go)
    def _():
        d2[...] = act(conv_sum("e2", "dec2b", 0, 384), "dec2b")

    up(d2, "up1", "u1")
    launch("u1")

    @pl.when(go)
    def _():
        late = conv_sum("u1", "dec1a", 0, 384, 1) + conv_sum("s1", "dec1a", 192, 384, 1, range(7, 9))
        acc1[...] = acc1[...] + late.reshape(acc1.shape)

    settle(SHARED[:-1])
    receive("u1")

    @pl.when(go)
    def _():
        ring_sum("u1", "dec1a", 0, 384, acc1)
        put("e1", act(acc1[...].reshape(1600, 192), "dec1a"), 1)
        clear_outside("e1")

    w_copy["dec1b"].wait()

    @pl.when(go)
    def _():
        d1[...] = act(conv_sum("e1", "dec1b", 0, 192), "dec1b")

    @pl.when(go)
    def _():
        out_channels = y_ref.shape[0]
        for hl in range(8):
            y_rows[:, hl, :] = rows_dot(w_head[...], d1[pl.ds(128 * hl, 128), :])
        k, n = iota((128, 128), 0), iota((128, 128), 1)
        pick = ((n >> 5) == ((k >> 2) & 3)) & ((n & 31) == 8 * (k & 3) + (k >> 4))
        y = jnp.dot(y_rows[...].reshape(8 * out_channels, 128), jnp.where(pick, 1.0, 0.0), precision=lax.Precision.HIGHEST,
                    preferred_element_type=F32).reshape(out_channels, 8, 128)
        for c in range(out_channels):
            for hb in range(4):
                y_ref[c, pl.ds(8 * hb, 8), :] = y[c, :, 32 * hb:32 * hb + 32] + b_head[c]

    settle(SHARED[-1:])


def solution(mesh):
    rows = mesh.shape["row"]
    cols = mesh.shape["col"]
    tile_spec = P(("data", "row"), "col", None)

    def device_body(image, *params):
        names = ("w_enc1a", "b_enc1a", "w_enc1b", "b_enc1b", "w_enc2a", "b_enc2a", "w_enc2b", "b_enc2b", "w_mid_a", "b_mid_a",
                 "w_mid_b", "b_mid_b", "w_up2", "w_dec2a", "b_dec2a", "w_dec2b", "b_dec2b", "w_up1", "w_dec1a", "b_dec1a",
                 "w_dec1b", "b_dec1b", "w_head", "b_head")
        p = dict(zip(names, params))
        high, wide, depth = image.shape
        weights = [p["w_" + n].swapaxes(2, 3) if n in TURNED else p["w_" + n] for n in WEIGHTS]
        weights = [w.reshape(-1, w.shape[-1]) for w in weights]
        biases = [p["b_" + n] for n in BIASES]
        vmem = pl.BlockSpec(memory_space=pltpu.VMEM)
        smem = pl.BlockSpec(memory_space=pltpu.SMEM)
        hbm = pl.BlockSpec(memory_space=pl.ANY)
        out_channels = p["w_head"].shape[1]
        smalls = [image.transpose(2, 0, 1), p["w_enc1a"].reshape(9, depth, -1), p["w_head"].T] + biases
        scratch = [pltpu.VMEM(a.shape, a.dtype) for a in smalls + weights]
        scratch += [pltpu.VMEM((s + 2 * r, s + 2 * r, 16, c), BF) for s, r, c in MAPS.values()]
        scratch += [pltpu.VMEM((4, tiles_of(n), 16, MAPS[n][2]), BF) for n in SHARED] * 2
        scratch += [pltpu.VMEM((4, 8, MAPS[n][2]), BF) for n in SHARED] * 2
        scratch += [pltpu.VMEM((10, 10, 16, 128), BF), pltpu.VMEM((128, 192), F32), pltpu.VMEM((64, 768), BF),
                    pltpu.VMEM((256, 384), BF), pltpu.VMEM((1024, 192), BF), pltpu.VMEM((10, 10, 16, 192), F32),
                    pltpu.VMEM((6, 6, 16, 384), F32), pltpu.VMEM((8, 8, 16, 192), F32), pltpu.VMEM((out_channels, 8, 128), F32)]
        scratch += [pltpu.SemaphoreType.DMA((len(SMALL),)), pltpu.SemaphoreType.DMA((len(WEIGHTS),)), pltpu.SemaphoreType.DMA((len(SHARED), 8)),
                    pltpu.SemaphoreType.DMA((len(SHARED), 8))]
        y = pl.pallas_call(
            functools.partial(body, rows, cols),
            out_shape=jax.ShapeDtypeStruct((out_channels, high, wide), F32),
            in_specs=[smem] + [hbm] * (len(smalls) + len(weights)),
            out_specs=vmem,
            scratch_shapes=scratch,
            compiler_params=pltpu.CompilerParams(collective_id=0, has_side_effects=True, vmem_limit_bytes=62 * 1024 * 1024),
            name="unet",
        )(p["b_head"], *smalls, *weights)
        return y.transpose(1, 2, 0)

    def program(image, *params):
        mapped = jax.shard_map(device_body, mesh=mesh, in_specs=(tile_spec,) + tuple([P()] * len(params)), out_specs=tile_spec, check_vma=False)
        return mapped(image, *params)

    return program
```
